32 devices in a mesh: freq: 4 (over y, x), shot: 8 (over z, core).
Axes of the slice: x: 2, y: 2, z: 4, core: 2. Of those that a mesh axis runs over, the one named last changes fastest.
Arguments:
- traces: bfloat16 [2, 4, 3072, 3072], P(None, 'freq', 'shot'), may hold values from -40 to 40, as said below
Outputs:
- multiples: bfloat16 [2, 4, 3072, 3072], P(None, 'freq', 'shot')
- primaries: bfloat16 [2, 4, 3072, 3072], P(None, 'freq', 'shot')
The draws below stay inside these ranges and needn't reach their ends.
Inputs may be any that keep to these rules, and one draw needn't show every extreme that they name: `traces`: finite recorded data.
All inputs are finite; a program needn't handle non-finite values.
Results may differ from the reference program's by a relative error of at most 0.0005.
Values may be sent and summed in bfloat16 or wider, within the bound.
A program may use at most 192 MiB of HBM per device.

```python
import math
import jax
import jax.numpy as jnp
from jax import lax

NRECV = 3072
FREQS = 4


def draw_traces(key, part):
    row_index = jnp.arange(NRECV, dtype=jnp.float32)
    row_ramp = jnp.sqrt(1.0 + 2.0 * row_index / (NRECV - 1))

    def per_band(freq_index):
        band_key = jax.random.fold_in(key, freq_index + 17)
        noise_key, scale_key = jax.random.split(band_key)
        noise = jnp.clip(jax.random.normal(noise_key, (2, NRECV, NRECV), jnp.float32), -4.0, 4.0)
        row_scale = jnp.exp(jax.random.uniform(scale_key, (NRECV,), jnp.float32, math.log(0.4), math.log(4.0)))
        base = noise * (0.3 * 0.70710678 * row_scale * row_ramp)[None, :, None]
        base_re = base[0]
        base_im = base[1]
        square_re = jnp.dot(base_re, base_re, precision=lax.Precision.HIGHEST) - jnp.dot(base_im, base_im, precision=lax.Precision.HIGHEST)
        square_im = jnp.dot(base_re, base_im, precision=lax.Precision.HIGHEST) + jnp.dot(base_im, base_re, precision=lax.Precision.HIGHEST)
        amplitude = 1.0 + 0.35 * freq_index.astype(jnp.float32) / (FREQS - 1)
        factor = 0.5 / math.sqrt(NRECV)
        return amplitude * jnp.stack([base_re + factor * square_re, base_im + factor * square_im])
    stacked = lax.map(per_band, jnp.arange(FREQS))
    return jnp.clip(jnp.transpose(stacked, (1, 0, 2, 3)), -40.0, 40.0).astype(jnp.bfloat16)


def setup_inputs(seed: int = 0) -> dict:
    seeds = jax.random.split(jax.random.key(seed), 2)
    traces = draw_traces(jax.random.fold_in(seeds[1], 71), 0)
    return dict(traces=traces)


epsilon = 1e-06

def reference(traces):
    factor = 1.0 / math.sqrt(NRECV)
    data = traces.astype(jnp.float32)

    def per_band(freq_index):
        data_re = data[0, freq_index]
        data_im = data[1, freq_index]
        mult_re = (jnp.dot(data_re, data_re, precision=lax.Precision.HIGHEST) - jnp.dot(data_im, data_im, precision=lax.Precision.HIGHEST)) * factor
        mult_im = (jnp.dot(data_re, data_im, precision=lax.Precision.HIGHEST) + jnp.dot(data_im, data_re, precision=lax.Precision.HIGHEST)) * factor
        return jnp.stack([mult_re, mult_im])
    mult = lax.map(per_band, jnp.arange(FREQS))
    mult = jnp.transpose(mult, (1, 0, 2, 3))
    mult_re = mult[0]
    mult_im = mult[1]
    data_re = data[0]
    data_im = data[1]
    total_count = float(FREQS * NRECV * NRECV)
    num_re = jnp.sum(mult_re * data_re + mult_im * data_im) / total_count
    num_im = jnp.sum(mult_re * data_im - mult_im * data_re) / total_count
    denom = jnp.sum(mult_re * mult_re + mult_im * mult_im) / total_count + epsilon
    fit_re = num_re / denom
    fit_im = num_im / denom
    prim_re = data_re - (fit_re * mult_re - fit_im * mult_im)
    prim_im = data_im - (fit_re * mult_im + fit_im * mult_re)
    primaries = jnp.stack([prim_re, prim_im]).astype(jnp.bfloat16)
    return (mult.astype(jnp.bfloat16), primaries)
```

```python
import functools
import math

import jax
import jax.numpy as jnp
from jax import lax
from jax.experimental import pallas as pl
from jax.experimental.pallas import tpu as pltpu
from jax.sharding import PartitionSpec as P

epsilon = 1e-06
MESH = pl.DeviceIdType.MESH
LANES = 128


def complex_product(left_re, left_im, right):
    left_block = jnp.stack(
        [jnp.concatenate([left_re, -left_im], axis=2), jnp.concatenate([left_im, left_re], axis=2)]
    )
    right_block = jnp.concatenate([right[0], right[1]], axis=1)
    return jnp.einsum("cfik,fkn->cfin", left_block, right_block, preferred_element_type=jnp.float32)


def finish(traces, mult_re, mult_im, num_re, num_im, denom):
    matrix_order = traces.shape[3]
    data_re = traces[0].astype(jnp.float32)
    data_im = traces[1].astype(jnp.float32)
    total_count = float(traces.shape[1] * lax.axis_size("freq") * matrix_order * matrix_order)
    scaled_den = denom / total_count + epsilon
    fit_re = num_re / total_count / scaled_den
    fit_im = num_im / total_count / scaled_den
    prim_re = data_re - (fit_re * mult_re - fit_im * mult_im)
    prim_im = data_im - (fit_re * mult_im + fit_im * mult_re)
    multiples = jnp.stack([mult_re, mult_im]).astype(jnp.bfloat16)
    primaries = jnp.stack([prim_re, prim_im]).astype(jnp.bfloat16)
    return (multiples, primaries)


def gathered(traces):
    factor = 1.0 / math.sqrt(traces.shape[3])
    products = complex_product(
        traces[0], traces[1], lax.all_gather(traces, "shot", axis=2, tiled=True)
    )
    mult_re = products[0] * factor
    mult_im = products[1] * factor
    data_re = traces[0].astype(jnp.float32)
    data_im = traces[1].astype(jnp.float32)
    sums = lax.psum(
        jnp.stack([
            jnp.sum(mult_re * data_re + mult_im * data_im),
            jnp.sum(mult_re * data_im - mult_im * data_re),
            jnp.sum(mult_re * mult_re + mult_im * mult_im),
        ]),
        ("freq", "shot"),
    )
    return finish(traces, mult_re, mult_im, sums[0], sums[1], sums[2])


def end_schedule(chunks, groups, ready):
    done = [0] * chunks
    pieces = []

    def column(c):
        if done[c] < groups:
            pieces.append((done[c], groups - done[c], c, 1))
            left = groups - done[c]
            done[c] = groups
            return left
        return 0

    window = 2 * groups
    room = window - column(0) - column(1)
    following = 2
    while min(done) < groups:
        while room > 0 and min(done) < groups:
            group = min(done)
            first = done.index(group)
            last = first
            while last < chunks and done[last] == group and last - first < room:
                last += 1
            pieces.append((group, 1, first, last - first))
            done[first:last] = [group + 1] * (last - first)
            room -= last - first
        room += window
        if following < chunks:
            room -= column(following)
            following += 1
    out = []
    for group, count, first, width in pieces:
        column_need = first - 2
        group_need = min(ready[g] for g in range(group, group + count))
        out.append((group, count, first, width, max(-1, min(column_need, group_need))))
    return tuple(out)


def line_kernel(
    chunks, kept, groups, ready, schedule, freqs,
    traces_ref, mult_ref, total_ref,
    grid, stage, acc, packed, partial_in,
    load_sem, piece_send, piece_recv, ici_recv, far_send, end_send, pair_send, pair_recv,
    result_send, result_recv, sum_send, sum_recv,
):
    rows = traces_ref.shape[2]
    order = traces_ref.shape[3]
    group_rows = rows // groups
    factor = 1.0 / math.sqrt(order)
    freq = lax.axis_index("freq")
    shot = lax.axis_index("shot")
    z = shot // 2
    core = shot % 2
    low = z < 2
    end = jnp.where(low, 0, 3)
    mid = jnp.where(low, 1, 2)
    far_mid = jnp.where(low, 2, 1)
    far_end = jnp.where(low, 3, 0)
    is_end = z == end
    beside = freq + 1 - 2 * (freq % 2)
    across = (freq + 2) % freqs

    def row(chip, plane):
        return pl.multiple_of((chip * 2 + plane) * rows, rows)

    def lane(j):
        return pl.multiple_of(j * LANES, LANES)

    def block(chip, plane, j):
        return grid.at[:, pl.ds(row(chip, plane), rows), pl.ds(lane(j), LANES)]

    def remote(src, dst, send, recv, chip, plane):
        return pltpu.make_async_remote_copy(
            src_ref=src, dst_ref=dst, send_sem=send, recv_sem=recv,
            device_id=(freq, chip * 2 + plane), device_id_type=MESH,
        )

    def ici(chip, j, send, slot, target):
        ref = block(chip, core, j)
        return remote(ref, ref, send, ici_recv.at[slot, j], target, core)

    def pair(chip, j, slot):
        ref = block(chip, core, j)
        return remote(ref, ref, pair_send.at[slot, j], pair_recv.at[slot, j], z, 1 - core)

    def arrived(chip, j, slot):
        ref = block(chip, core, j)
        remote(ref, ref, far_send.at[0, j], ici_recv.at[slot, j], z, 1 - core).wait_recv()

    def paired(chip, j, slot):
        ref = block(chip, 1 - core, j)
        remote(ref, ref, pair_send.at[slot, j], pair_recv.at[slot, j], z, 1 - core).wait_recv()

    def to_end(chip, j, slot):
        return ici(chip, j, end_send.at[slot, j], slot, end)

    def to_far(chip, j, slot):
        return ici(chip, j, far_send.at[slot, j], slot + 1, far_mid)

    def piece(d):
        group, count, first, width, _ = schedule[d]
        ref = grid.at[
            :,
            pl.ds(pl.multiple_of(row(end, core) + group * group_rows, group_rows), count * group_rows),
            pl.ds(first * LANES, width * LANES),
        ]
        return remote(ref, ref, piece_send.at[d], piece_recv.at[d], mid, core)

    def result(g, j):
        here = pl.ds(pl.multiple_of(g * group_rows, group_rows), group_rows)
        return remote(
            stage.at[:, here, pl.ds(lane(j - kept), LANES)],
            mult_ref.at[:, here, pl.ds(lane(j), LANES)],
            result_send.at[g, j], result_recv.at[g, j], end, core,
        )

    def multiply(first, count, j, out, out_row, out_lane):
        here = pl.ds(first, count)
        column = pl.ds(lane(j), LANES)
        right = jnp.concatenate([grid[0, :, column], grid[1, :, column]], axis=1)
        by_re = jnp.dot(grid[0, here, :], right, preferred_element_type=jnp.float32)
        by_im = jnp.dot(grid[1, here, :], right, preferred_element_type=jnp.float32)
        mult_re = (by_re[:, :LANES] - by_im[:, LANES:]) * factor
        mult_im = (by_re[:, LANES:] + by_im[:, :LANES]) * factor
        out[0, pl.ds(out_row, count), pl.ds(out_lane, LANES)] = mult_re
        out[1, pl.ds(out_row, count), pl.ds(out_lane, LANES)] = mult_im
        data_re = grid[0, here, column].astype(jnp.float32)
        data_im = grid[1, here, column].astype(jnp.float32)
        for i, term in enumerate((
            mult_re * data_re + mult_im * data_im,
            mult_re * data_im - mult_im * data_re,
            mult_re * mult_re + mult_im * mult_im,
        )):
            acc[pl.ds(i * 8, 8), :] += jnp.sum(term.reshape(count // 8, 8, LANES), axis=0)

    def own(j):
        multiply(row(z, core), rows, j, mult_ref, 0, lane(j))

    def loop(lower, upper, body):
        def run(j, carry):
            body(j)
            return carry
        lax.fori_loop(lower, upper, run, 0)

    def pack():
        sums = [jnp.sum(acc[pl.ds(8 * i, 8), :], axis=0, keepdims=True) for i in range(3)]
        return jnp.concatenate(sums + [jnp.zeros((5, LANES), jnp.float32)], axis=0)

    def give(slot, device):
        return pltpu.make_async_remote_copy(
            src_ref=packed.at[slot], dst_ref=partial_in.at[slot],
            send_sem=sum_send.at[slot], recv_sem=sum_recv.at[slot],
            device_id=device, device_id_type=MESH,
        )

    def give_total():
        return remote(total_ref, total_ref, sum_send.at[5], sum_recv.at[5], end, core)

    mine = grid.at[:, pl.ds(row(z, core), rows), :]
    load = pltpu.make_async_copy(traces_ref.at[:, 0], mine, load_sem)
    load.start()
    acc[...] = jnp.zeros_like(acc)

    barrier = pltpu.get_barrier_semaphore()

    def greet(f, s):
        pl.semaphore_signal(barrier, inc=1, device_id=(f, s), device_id_type=MESH)

    greet(freq, z * 2 + 1 - core)

    @pl.when(is_end)
    def _():
        greet(freq, mid * 2 + core)
        pl.semaphore_wait(barrier, 2)

    @pl.when(jnp.logical_not(is_end))
    def _():
        greet(freq, end * 2 + core)
        greet(freq, far_mid * 2 + core)
        greet(beside, shot)
        greet(across, shot)
        pl.semaphore_wait(barrier, 5)

    load.wait()

    @pl.when(is_end)
    def _():
        for d in range(len(schedule)):
            piece(d).start()
        loop(0, kept, lambda j: pair(z, j, 3).start())

        def work(j):
            for slot, chip in enumerate((mid, far_mid, far_end)):
                arrived(chip, j, slot)
                pair(chip, j, slot).start()
            for slot, chip in enumerate((mid, far_mid, far_end, end)):
                paired(chip, j, slot)
            own(j)

        loop(0, kept, work)
        packed[0] = pack()
        give(0, (freq, mid * 2 + core)).start()

        def settle(j):
            for slot, chip in enumerate((mid, far_mid, far_end, end)):
                pair(chip, j, slot).wait_send()

        loop(0, kept, settle)
        for d in range(len(schedule)):
            piece(d).wait_send()
        give(0, (freq, mid * 2 + core)).wait_send()

        def take(j):
            loop(0, groups, lambda g: result(g, j).wait_recv())

        loop(kept, chunks, take)
        give_total().wait_recv()

    @pl.when(jnp.logical_not(is_end))
    def _():
        def own_sends(j):
            to_far(z, j, 0).start()

            @pl.when(j < kept)
            def _():
                to_end(z, j, 0).start()
            pair(z, j, 3).start()

        def near(j):
            to_far(end, j, 1).start()
            pair(end, j, 0).start()

        def take_pieces(i):
            for d in range(len(schedule)):
                @pl.when(i == schedule[d][4])
                def _(d=d):
                    piece(d).wait_recv()

        own_sends(0)
        own_sends(1)
        for d in range(len(schedule)):
            if schedule[d][4] < 0:
                piece(d).wait_recv()
        near(0)
        near(1)

        def work(j):
            for slot, chip in ((1, far_mid), (2, far_end)):
                arrived(chip, j, slot)

                @pl.when(j < kept)
                def _():
                    to_end(chip, j, slot).start()
                pair(chip, j, slot).start()
            take_pieces(j)

            @pl.when(j + 2 < chunks)
            def _():
                own_sends(j + 2)
                near(j + 2)
            for slot, chip in ((0, end), (1, far_mid), (2, far_end), (3, z)):
                paired(chip, j, slot)

            def group(g):
                at = ready[0]
                for k in range(1, groups):
                    at = jnp.where(g >= k, ready[k], at)
                lower = jnp.where(j == at, kept, j)
                upper = jnp.where(j >= at, j + 1, lower)

                def task(jj):
                    multiply(
                        pl.multiple_of(row(end, core) + g * group_rows, group_rows), group_rows, jj,
                        stage, pl.multiple_of(g * group_rows, group_rows), lane(jj - kept),
                    )
                    result(g, jj).start()

                loop(lower, upper, task)

            loop(0, groups, group)
            own(j)

        loop(0, chunks, work)

        give(0, (freq, end * 2 + core)).wait_recv()
        total = pack() + partial_in[0]
        for slot, device in enumerate((
            (freq, z * 2 + 1 - core), (freq, far_mid * 2 + core), (beside, shot), (across, shot),
        )):
            packed[slot + 1] = total
            give(slot + 1, device).start()
            give(slot + 1, device).wait_recv()
            total = total + partial_in[slot + 1]
        total_ref[...] = total
        give_total().start()

        def drain(j):
            to_far(z, j, 0).wait_send()
            to_far(end, j, 1).wait_send()
            for slot, chip in enumerate((end, far_mid, far_end, z)):
                pair(chip, j, slot).wait_send()

            @pl.when(j < kept)
            def _():
                for slot, chip in enumerate((z, far_mid, far_end)):
                    to_end(chip, j, slot).wait_send()

            @pl.when(j >= kept)
            def _():
                loop(0, groups, lambda g: result(g, j).wait_send())

        loop(0, chunks, drain)
        for slot, device in enumerate((
            (freq, z * 2 + 1 - core), (freq, far_mid * 2 + core), (beside, shot), (across, shot),
        )):
            give(slot + 1, device).wait_send()
        give_total().wait_send()


def epilogue_kernel(
    total_count, strip, width, total_ref, traces_ref, mult_ref, multiples_ref, primaries_ref,
    multiples, primaries, fit, sems,
):
    rows, order = mult_ref.shape[1], mult_ref.shape[2]
    num_re, num_im, denom = (jnp.sum(total_ref[pl.ds(i, 1), :]) for i in range(3))
    scaled_den = denom / total_count + epsilon
    fit_re = num_re / total_count / scaled_den
    fit_im = num_im / total_count / scaled_den

    def copies(s):
        here = pl.ds(pl.multiple_of(s * strip, strip), strip)
        return (
            pltpu.make_async_copy(multiples.at[:, here, :], multiples_ref.at[:, 0, here, :], sems.at[0, s]),
            pltpu.make_async_copy(primaries.at[:, here, :], primaries_ref.at[:, 0, here, :], sems.at[1, s]),
        )

    def part(s, carry):
        here = pl.ds(pl.multiple_of(s * strip, strip), strip)
        for q in range(order // width):
            columns = pl.ds(q * width, width)
            mult_re = mult_ref[0, here, columns]
            mult_im = mult_ref[1, here, columns]
            data_re = traces_ref[0, 0, here, columns].astype(jnp.float32)
            data_im = traces_ref[1, 0, here, columns].astype(jnp.float32)
            prim_re = data_re - (fit_re * mult_re - fit_im * mult_im)
            prim_im = data_im - (fit_re * mult_im + fit_im * mult_re)
            multiples[0, here, columns] = mult_re.astype(jnp.bfloat16)
            multiples[1, here, columns] = mult_im.astype(jnp.bfloat16)
            primaries[0, here, columns] = prim_re.astype(jnp.bfloat16)
            primaries[1, here, columns] = prim_im.astype(jnp.bfloat16)
        for copy in copies(s):
            copy.start()
        return carry

    lax.fori_loop(0, rows // strip, part, 0)

    def wait(s, carry):
        for copy in copies(s):
            copy.wait()
        return carry

    lax.fori_loop(0, rows // strip, wait, 0)


def on_a_line(traces):
    rows, order = traces.shape[2], traces.shape[3]
    freqs = lax.axis_size("freq")
    chunks = order // LANES
    groups = 3
    kept = max(1, round(0.22 * chunks))
    ready = tuple(max(kept, round(f * chunks)) for f in (0.29, 0.42, 0.5))
    schedule = end_schedule(chunks, groups, ready)
    pieces = len(schedule)
    dma = pltpu.SemaphoreType.DMA
    mult, totals = pl.pallas_call(
        functools.partial(line_kernel, chunks, kept, groups, ready, schedule, freqs),
        out_shape=(
            pltpu.VMEM((2, rows, order), jnp.float32),
            pltpu.VMEM((8, LANES), jnp.float32),
        ),
        in_specs=[pl.BlockSpec(memory_space=pltpu.HBM)],
        out_specs=(
            pl.BlockSpec(memory_space=pltpu.VMEM),
            pl.BlockSpec(memory_space=pltpu.VMEM),
        ),
        scratch_shapes=[
            pltpu.VMEM((2, order, order), jnp.bfloat16),
            pltpu.VMEM((2, rows, (chunks - kept) * LANES), jnp.float32),
            pltpu.VMEM((24, LANES), jnp.float32),
            pltpu.VMEM((5, 8, LANES), jnp.float32),
            pltpu.VMEM((5, 8, LANES), jnp.float32),
            dma, dma((pieces,)), dma((pieces,)), dma((3, chunks)), dma((2, chunks)),
            dma((3, kept)), dma((4, chunks)), dma((4, chunks)),
            dma((groups, chunks)), dma((groups, chunks)), dma((6,)), dma((6,)),
        ],
        compiler_params=pltpu.CompilerParams(
            collective_id=0, has_side_effects=True, vmem_limit_bytes=48 * 1024 * 1024
        ),
    )(traces)
    strip = 16
    out = jax.ShapeDtypeStruct(traces.shape, traces.dtype)
    whole = pl.BlockSpec(memory_space=pltpu.VMEM)
    away = pl.BlockSpec(memory_space=pltpu.HBM)
    return pl.pallas_call(
        functools.partial(epilogue_kernel, float(freqs * order * order), strip, 4 * LANES),
        out_shape=(out, out),
        in_specs=[whole, whole, whole],
        out_specs=(away, away),
        scratch_shapes=[
            pltpu.VMEM((2, rows, order), jnp.bfloat16),
            pltpu.VMEM((2, rows, order), jnp.bfloat16),
            pltpu.SMEM((2,), jnp.float32),
            dma((2, rows // strip)),
        ],
        compiler_params=pltpu.CompilerParams(vmem_limit_bytes=24 * 1024 * 1024),
    )(totals, traces, mult)


def solution(mesh):
    placed = P(None, "freq", "shot", None)

    def per_device(traces):
        four_chips = mesh.shape["shot"] == 2 * 4 and mesh.shape["freq"] == 4
        rows, order = traces.shape[2], traces.shape[3]
        fits = rows % 48 == 0 and order % (4 * LANES) == 0
        if four_chips and traces.shape[1] == 1 and fits:
            return on_a_line(traces)
        return gathered(traces)

    return jax.shard_map(
        per_device, mesh=mesh, in_specs=(placed,), out_specs=(placed, placed), check_vma=False
    )
```

```python
import functools
import math

import jax
import jax.numpy as jnp
from jax import lax
from jax.experimental import pallas as pl
from jax.experimental.pallas import tpu as pltpu
from jax.sharding import PartitionSpec as P

epsilon = 1e-06
MESH = pl.DeviceIdType.MESH
LANES = 128


def complex_product(left_re, left_im, right):
    left_block = jnp.stack(
        [jnp.concatenate([left_re, -left_im], axis=2), jnp.concatenate([left_im, left_re], axis=2)]
    )
    right_block = jnp.concatenate([right[0], right[1]], axis=1)
    return jnp.einsum("cfik,fkn->cfin", left_block, right_block, preferred_element_type=jnp.float32)


def finish(traces, mult_re, mult_im, num_re, num_im, denom):
    matrix_order = traces.shape[3]
    data_re = traces[0].astype(jnp.float32)
    data_im = traces[1].astype(jnp.float32)
    total_count = float(traces.shape[1] * lax.axis_size("freq") * matrix_order * matrix_order)
    scaled_den = denom / total_count + epsilon
    fit_re = num_re / total_count / scaled_den
    fit_im = num_im / total_count / scaled_den
    prim_re = data_re - (fit_re * mult_re - fit_im * mult_im)
    prim_im = data_im - (fit_re * mult_im + fit_im * mult_re)
    multiples = jnp.stack([mult_re, mult_im]).astype(jnp.bfloat16)
    primaries = jnp.stack([prim_re, prim_im]).astype(jnp.bfloat16)
    return (multiples, primaries)


def gathered(traces):
    factor = 1.0 / math.sqrt(traces.shape[3])
    products = complex_product(
        traces[0], traces[1], lax.all_gather(traces, "shot", axis=2, tiled=True)
    )
    mult_re = products[0] * factor
    mult_im = products[1] * factor
    data_re = traces[0].astype(jnp.float32)
    data_im = traces[1].astype(jnp.float32)
    sums = lax.psum(
        jnp.stack([
            jnp.sum(mult_re * data_re + mult_im * data_im),
            jnp.sum(mult_re * data_im - mult_im * data_re),
            jnp.sum(mult_re * mult_re + mult_im * mult_im),
        ]),
        ("freq", "shot"),
    )
    return finish(traces, mult_re, mult_im, sums[0], sums[1], sums[2])


def end_schedule(chunks, groups, ready):
    half, most = chunks // 2, 3 * chunks // 4
    done = [0] * chunks
    pieces = []

    def column(c):
        left = groups - done[c]
        if left:
            pieces.append((done[c], left, c, 1))
            done[c] = groups
        return left

    window = 2 * groups
    room = window - column(0) - column(1)
    following = 2
    while min(done[:most]) < groups:
        while room > 0 and min(done[:most]) < groups:
            group = min(done[:most])
            first = done.index(group)
            bound = half if first < half else most
            last = first
            while last < bound and done[last] == group and last - first < room:
                last += 1
            pieces.append((group, 1, first, last - first))
            done[first:last] = [group + 1] * (last - first)
            room -= last - first
        room += window
        if following < chunks:
            room -= column(following)
            following += 1
    step = max(1, (chunks - most) // 2)
    pieces += [(0, groups, c, min(step, chunks - c)) for c in range(most, chunks, step)]
    out = []
    for group, count, first, width in pieces:
        column_need = 2 * (first - 2) + 1
        group_need = min(2 * ready[g] for g in range(group, group + count)) if first < most else chunks - 1
        out.append((group, count, first, width, max(-1, min(column_need, group_need, chunks - 1))))
    return tuple(out)


def line_kernel(
    chunks, kept, groups, ready, schedule, freqs,
    traces_ref, mult_ref, total_ref,
    grid, stage, acc, packed, partial_in,
    load_sem, piece_send, piece_recv, ici_recv, far_send, end_send, pair_send, pair_recv,
    result_send, result_recv, full_send, full_recv, sum_send, sum_recv,
):
    rows = traces_ref.shape[2]
    order = traces_ref.shape[3]
    group_rows = rows // groups
    half, quarter = chunks // 2, chunks // 4
    factor = 1.0 / math.sqrt(order)
    freq = lax.axis_index("freq")
    shot = lax.axis_index("shot")
    z = shot // 2
    core = shot % 2
    low = z < 2
    end = jnp.where(low, 0, 3)
    mid = jnp.where(low, 1, 2)
    far_mid = jnp.where(low, 2, 1)
    far_end = jnp.where(low, 3, 0)
    is_end = z == end
    beside = freq + 1 - 2 * (freq % 2)
    across = (freq + 2) % freqs

    def first_last(i):
        return (i + quarter) % chunks

    def first_third(i):
        return jnp.where(i < half, i + quarter, jnp.where(i < 3 * quarter, i - half, i))

    def sent(i):
        return jnp.where(low, first_last(i), first_third(i))

    def taken(i):
        return jnp.where(low, first_third(i), first_last(i))

    def row(chip, plane):
        return pl.multiple_of((chip * 2 + plane) * rows, rows)

    def lane(j):
        return pl.multiple_of(j * LANES, LANES)

    def block(chip, plane, j):
        return grid.at[:, pl.ds(row(chip, plane), rows), pl.ds(lane(j), LANES)]

    def remote(src, dst, send, recv, chip, plane):
        return pltpu.make_async_remote_copy(
            src_ref=src, dst_ref=dst, send_sem=send, recv_sem=recv,
            device_id=(freq, chip * 2 + plane), device_id_type=MESH,
        )

    def ici(chip, j, send, slot, target):
        ref = block(chip, core, j)
        return remote(ref, ref, send, ici_recv.at[slot, j], target, core)

    def pair(chip, j, slot):
        ref = block(chip, core, j)
        return remote(ref, ref, pair_send.at[slot, j], pair_recv.at[slot, j], z, 1 - core)

    def arrived(chip, j, slot):
        ref = block(chip, core, j)
        remote(ref, ref, far_send.at[0, j], ici_recv.at[slot, j], z, 1 - core).wait_recv()

    def paired(chip, j, slot):
        ref = block(chip, 1 - core, j)
        remote(ref, ref, pair_send.at[slot, j], pair_recv.at[slot, j], z, 1 - core).wait_recv()

    def to_end(chip, j, slot):
        return ici(chip, j, end_send.at[slot, j], slot, end)

    def to_far(chip, j, slot):
        return ici(chip, j, far_send.at[slot, j], slot + 1, far_mid)

    def piece(d):
        group, count, first, width, _ = schedule[d]
        ref = grid.at[
            :,
            pl.ds(pl.multiple_of(row(end, core) + group * group_rows, group_rows), count * group_rows),
            pl.ds(lane(sent(first)), width * LANES),
        ]
        return remote(ref, ref, piece_send.at[d], piece_recv.at[d], mid, core)

    def result(g, i):
        here = pl.ds(pl.multiple_of(g * group_rows, group_rows), group_rows)
        return remote(
            stage.at[:, here, pl.ds(lane(i - kept), LANES)],
            mult_ref.at[:, here, pl.ds(lane(taken(i)), LANES)],
            result_send.at[g, i], result_recv.at[g, i], end, core,
        )

    def full(i):
        return remote(
            stage.at[:, :, pl.ds(lane(i - kept), LANES)],
            mult_ref.at[:, :, pl.ds(lane(taken(i)), LANES)],
            full_send.at[i - half], full_recv.at[i - half], end, core,
        )

    def multiply(first, count, j, inner, depth, out, out_row, out_lane, onto, fit):
        here = pl.ds(first, count)
        column = pl.ds(lane(j), LANES)
        span = pl.ds(inner, depth)
        right = jnp.concatenate([grid[0, span, column], grid[1, span, column]], axis=1)
        by_re = jnp.dot(grid[0, here, span], right, preferred_element_type=jnp.float32)
        by_im = jnp.dot(grid[1, here, span], right, preferred_element_type=jnp.float32)
        mult_re = (by_re[:, :LANES] - by_im[:, LANES:]) * factor
        mult_im = (by_re[:, LANES:] + by_im[:, :LANES]) * factor
        to = pl.ds(out_row, count), pl.ds(out_lane, LANES)
        if onto:
            mult_re = mult_re + out[0, to[0], to[1]]
            mult_im = mult_im + out[1, to[0], to[1]]
        out[0, to[0], to[1]] = mult_re
        out[1, to[0], to[1]] = mult_im
        if not fit:
            return
        data_re = grid[0, here, column].astype(jnp.float32)
        data_im = grid[1, here, column].astype(jnp.float32)
        for i, term in enumerate((
            mult_re * data_re + mult_im * data_im,
            mult_re * data_im - mult_im * data_re,
            mult_re * mult_re + mult_im * mult_im,
        )):
            acc[pl.ds(i * 8, 8), :] += jnp.sum(term.reshape(count // 8, 8, LANES), axis=0)

    def own(j):
        multiply(row(z, core), rows, j, 0, order, mult_ref, 0, lane(j), False, True)

    def loop(lower, upper, body):
        def run(j, carry):
            body(j)
            return carry
        lax.fori_loop(lower, upper, run, 0)

    def pack():
        sums = [jnp.sum(acc[pl.ds(8 * i, 8), :], axis=0, keepdims=True) for i in range(3)]
        return jnp.concatenate(sums + [jnp.zeros((5, LANES), jnp.float32)], axis=0)

    def give(slot, device):
        return pltpu.make_async_remote_copy(
            src_ref=packed.at[slot], dst_ref=partial_in.at[slot],
            send_sem=sum_send.at[slot], recv_sem=sum_recv.at[slot],
            device_id=device, device_id_type=MESH,
        )

    def give_total():
        return remote(total_ref, total_ref, sum_send.at[5], sum_recv.at[5], end, core)

    mine = grid.at[:, pl.ds(row(z, core), rows), :]
    load = pltpu.make_async_copy(traces_ref.at[:, 0], mine, load_sem)
    load.start()
    acc[...] = jnp.zeros_like(acc)

    barrier = pltpu.get_barrier_semaphore()

    def greet(f, s):
        pl.semaphore_signal(barrier, inc=1, device_id=(f, s), device_id_type=MESH)

    greet(freq, z * 2 + 1 - core)

    @pl.when(is_end)
    def _():
        greet(freq, mid * 2 + core)
        pl.semaphore_wait(barrier, 2)

    @pl.when(jnp.logical_not(is_end))
    def _():
        greet(freq, end * 2 + core)
        greet(freq, far_mid * 2 + core)
        greet(beside, shot)
        greet(across, shot)
        pl.semaphore_wait(barrier, 5)

    load.wait()

    @pl.when(is_end)
    def _():
        for d in range(len(schedule)):
            piece(d).start()
        loop(0, half, lambda i: pair(z, taken(i), 3).start())

        def work(i):
            j = taken(i)
            for slot, chip in enumerate((mid, far_mid, far_end)):
                arrived(chip, j, slot)
                pair(chip, j, slot).start()
            for slot, chip in enumerate((mid, far_mid, far_end, end)):
                paired(chip, j, slot)
            own(j)

        loop(0, kept, work)

        def complete(i):
            j = taken(i)
            paired(end, j, 3)
            loop(0, groups, lambda g: result(g, i).wait_recv())
            inner = pl.multiple_of(end * 2 * rows, 2 * rows)
            multiply(row(z, core), rows, j, inner, 2 * rows, mult_ref, 0, lane(j), True, True)

        loop(kept, half, complete)
        packed[0] = pack()
        give(0, (freq, mid * 2 + core)).start()

        def settle(i):
            pair(z, taken(i), 3).wait_send()

            @pl.when(i < kept)
            def _():
                for slot, chip in enumerate((mid, far_mid, far_end)):
                    pair(chip, taken(i), slot).wait_send()

        loop(0, half, settle)
        for d in range(len(schedule)):
            piece(d).wait_send()
        give(0, (freq, mid * 2 + core)).wait_send()
        loop(half, chunks, lambda i: full(i).wait_recv())
        give_total().wait_recv()

    @pl.when(jnp.logical_not(is_end))
    def _():
        def own_sends(i):
            to_far(z, sent(i), 0).start()

            @pl.when(i < kept)
            def _():
                to_end(z, taken(i), 0).start()
            pair(z, taken(i), 3).start()

        def near(i):
            to_far(end, sent(i), 1).start()

            @pl.when(i < half)
            def _():
                pair(end, sent(i), 0).start()

        def take_pieces(stop):
            for d in range(len(schedule)):
                @pl.when(stop == schedule[d][4])
                def _(d=d):
                    piece(d).wait_recv()

        own_sends(0)
        own_sends(1)
        for d in range(len(schedule)):
            if schedule[d][4] < 0:
                piece(d).wait_recv()
        near(0)
        near(1)

        inner = pl.multiple_of((1 - end // 3) * 2 * rows, 2 * rows)

        def part(g, i):
            first = pl.multiple_of(g * group_rows, group_rows)
            multiply(
                pl.multiple_of(row(end, core) + first, group_rows), group_rows, taken(i),
                inner, order - 2 * rows, stage, first, lane(i - kept), False, False,
            )
            result(g, i).start()

        def starts(g):
            at = ready[0]
            for k in range(1, groups):
                at = jnp.where(g >= k, ready[k], at)
            return at

        def parts(i, step):
            def group(g):
                at = starts(g)
                if step == 0:
                    lower, upper = kept, jnp.where(i == at, i, kept)
                else:
                    lower, upper = i, jnp.where(jnp.logical_and(i >= at, i < half), i + 1, i)
                loop(lower, upper, lambda ii: part(g, ii))

            loop(0, groups, group)

        def work(i):
            take_pieces(2 * i)
            for step in range(2):
                if step == 1:
                    j = taken(i)
                    for slot, chip in ((1, far_mid), (2, far_end)):
                        arrived(chip, j, slot)

                        @pl.when(i < kept)
                        def _(slot=slot, chip=chip):
                            to_end(chip, j, slot).start()
                        pair(chip, j, slot).start()
                    take_pieces(2 * i + 1)

                    @pl.when(i + 2 < chunks)
                    def _():
                        own_sends(i + 2)
                        near(i + 2)

                    @pl.when(i == half - 1)
                    def _():
                        loop(half, chunks, lambda ii: pair(end, sent(ii), 0).start())
                    for slot, chip in ((0, end), (1, far_mid), (2, far_end), (3, z)):
                        paired(chip, j, slot)
                parts(i, step)

            @pl.when(i >= half)
            def _():
                multiply(row(end, core), rows, j, 0, order, stage, 0, lane(i - kept), False, True)
                full(i).start()
            own(j)

        loop(0, chunks, work)

        give(0, (freq, end * 2 + core)).wait_recv()
        total = pack() + partial_in[0]
        for slot, device in enumerate((
            (freq, z * 2 + 1 - core), (freq, far_mid * 2 + core), (beside, shot), (across, shot),
        )):
            packed[slot + 1] = total
            give(slot + 1, device).start()
            give(slot + 1, device).wait_recv()
            total = total + partial_in[slot + 1]
        total_ref[...] = total
        give_total().start()

        def drain(i):
            to_far(z, sent(i), 0).wait_send()
            to_far(end, sent(i), 1).wait_send()
            for slot, chip in enumerate((end, far_mid, far_end, z)):
                pair(chip, taken(i), slot).wait_send()

            @pl.when(i < kept)
            def _():
                for slot, chip in enumerate((z, far_mid, far_end)):
                    to_end(chip, taken(i), slot).wait_send()

            @pl.when(jnp.logical_and(i >= kept, i < half))
            def _():
                loop(0, groups, lambda g: result(g, i).wait_send())

            @pl.when(i >= half)
            def _():
                full(i).wait_send()

        loop(0, chunks, drain)
        for slot, device in enumerate((
            (freq, z * 2 + 1 - core), (freq, far_mid * 2 + core), (beside, shot), (across, shot),
        )):
            give(slot + 1, device).wait_send()
        give_total().wait_send()


def epilogue_kernel(
    total_count, strip, width, total_ref, traces_ref, mult_ref, multiples_ref, primaries_ref,
    multiples, primaries, fit, sems,
):
    rows, order = mult_ref.shape[1], mult_ref.shape[2]
    num_re, num_im, denom = (jnp.sum(total_ref[pl.ds(i, 1), :]) for i in range(3))
    scaled_den = denom / total_count + epsilon
    fit_re = num_re / total_count / scaled_den
    fit_im = num_im / total_count / scaled_den

    def copies(s):
        here = pl.ds(pl.multiple_of(s * strip, strip), strip)
        return (
            pltpu.make_async_copy(multiples.at[:, here, :], multiples_ref.at[:, 0, here, :], sems.at[0, s]),
            pltpu.make_async_copy(primaries.at[:, here, :], primaries_ref.at[:, 0, here, :], sems.at[1, s]),
        )

    def part(s, carry):
        here = pl.ds(pl.multiple_of(s * strip, strip), strip)
        for q in range(order // width):
            columns = pl.ds(q * width, width)
            mult_re = mult_ref[0, here, columns]
            mult_im = mult_ref[1, here, columns]
            data_re = traces_ref[0, 0, here, columns].astype(jnp.float32)
            data_im = traces_ref[1, 0, here, columns].astype(jnp.float32)
            prim_re = data_re - (fit_re * mult_re - fit_im * mult_im)
            prim_im = data_im - (fit_re * mult_im + fit_im * mult_re)
            multiples[0, here, columns] = mult_re.astype(jnp.bfloat16)
            multiples[1, here, columns] = mult_im.astype(jnp.bfloat16)
            primaries[0, here, columns] = prim_re.astype(jnp.bfloat16)
            primaries[1, here, columns] = prim_im.astype(jnp.bfloat16)
        for copy in copies(s):
            copy.start()
        return carry

    lax.fori_loop(0, rows // strip, part, 0)

    def wait(s, carry):
        for copy in copies(s):
            copy.wait()
        return carry

    lax.fori_loop(0, rows // strip, wait, 0)


def on_a_line(traces):
    rows, order = traces.shape[2], traces.shape[3]
    freqs = lax.axis_size("freq")
    chunks = order // LANES
    groups = 3
    half = chunks // 2
    kept = max(1, round(0.21 * chunks))
    ready = tuple(min(half - 1, max(kept, round(f * chunks))) for f in (0.2, 0.29, 0.34))
    schedule = end_schedule(chunks, groups, ready)
    pieces = len(schedule)
    dma = pltpu.SemaphoreType.DMA
    mult, totals = pl.pallas_call(
        functools.partial(line_kernel, chunks, kept, groups, ready, schedule, freqs),
        out_shape=(
            pltpu.VMEM((2, rows, order), jnp.float32),
            pltpu.VMEM((8, LANES), jnp.float32),
        ),
        in_specs=[pl.BlockSpec(memory_space=pltpu.HBM)],
        out_specs=(
            pl.BlockSpec(memory_space=pltpu.VMEM),
            pl.BlockSpec(memory_space=pltpu.VMEM),
        ),
        scratch_shapes=[
            pltpu.VMEM((2, order, order), jnp.bfloat16),
            pltpu.VMEM((2, rows, (chunks - kept) * LANES), jnp.float32),
            pltpu.VMEM((24, LANES), jnp.float32),
            pltpu.VMEM((5, 8, LANES), jnp.float32),
            pltpu.VMEM((5, 8, LANES), jnp.float32),
            dma, dma((pieces,)), dma((pieces,)), dma((3, chunks)), dma((2, chunks)),
            dma((3, chunks)), dma((4, chunks)), dma((4, chunks)),
            dma((groups, half)), dma((groups, half)), dma((half,)), dma((half,)), dma((6,)), dma((6,)),
        ],
        compiler_params=pltpu.CompilerParams(
            collective_id=0, has_side_effects=True, vmem_limit_bytes=48 * 1024 * 1024
        ),
    )(traces)
    strip = 16
    out = jax.ShapeDtypeStruct(traces.shape, traces.dtype)
    whole = pl.BlockSpec(memory_space=pltpu.VMEM)
    away = pl.BlockSpec(memory_space=pltpu.HBM)
    return pl.pallas_call(
        functools.partial(epilogue_kernel, float(freqs * order * order), strip, 4 * LANES),
        out_shape=(out, out),
        in_specs=[whole, whole, whole],
        out_specs=(away, away),
        scratch_shapes=[
            pltpu.VMEM((2, rows, order), jnp.bfloat16),
            pltpu.VMEM((2, rows, order), jnp.bfloat16),
            pltpu.SMEM((2,), jnp.float32),
            dma((2, rows // strip)),
        ],
        compiler_params=pltpu.CompilerParams(vmem_limit_bytes=24 * 1024 * 1024),
    )(totals, traces, mult)


def solution(mesh):
    placed = P(None, "freq", "shot", None)

    def per_device(traces):
        four_chips = mesh.shape["shot"] == 2 * 4 and mesh.shape["freq"] == 4
        rows, order = traces.shape[2], traces.shape[3]
        fits = rows % 48 == 0 and order % (4 * LANES) == 0
        if four_chips and traces.shape[1] == 1 and fits:
            return on_a_line(traces)
        return gathered(traces)

    return jax.shard_map(
        per_device, mesh=mesh, in_specs=(placed,), out_specs=(placed, placed), check_vma=False
    )
```

```python
import functools
import math

import jax
import jax.numpy as jnp
from jax import lax
from jax.experimental import pallas as pl
from jax.experimental.pallas import tpu as pltpu
from jax.sharding import PartitionSpec as P

epsilon = 1e-06
MESH = pl.DeviceIdType.MESH
LANES = 128


def complex_product(left_re, left_im, right):
    left_block = jnp.stack(
        [jnp.concatenate([left_re, -left_im], axis=2), jnp.concatenate([left_im, left_re], axis=2)]
    )
    right_block = jnp.concatenate([right[0], right[1]], axis=1)
    return jnp.einsum("cfik,fkn->cfin", left_block, right_block, preferred_element_type=jnp.float32)


def finish(traces, mult_re, mult_im, num_re, num_im, denom):
    matrix_order = traces.shape[3]
    data_re = traces[0].astype(jnp.float32)
    data_im = traces[1].astype(jnp.float32)
    total_count = float(traces.shape[1] * lax.axis_size("freq") * matrix_order * matrix_order)
    scaled_den = denom / total_count + epsilon
    fit_re = num_re / total_count / scaled_den
    fit_im = num_im / total_count / scaled_den
    prim_re = data_re - (fit_re * mult_re - fit_im * mult_im)
    prim_im = data_im - (fit_re * mult_im + fit_im * mult_re)
    multiples = jnp.stack([mult_re, mult_im]).astype(jnp.bfloat16)
    primaries = jnp.stack([prim_re, prim_im]).astype(jnp.bfloat16)
    return (multiples, primaries)


def gathered(traces):
    factor = 1.0 / math.sqrt(traces.shape[3])
    products = complex_product(
        traces[0], traces[1], lax.all_gather(traces, "shot", axis=2, tiled=True)
    )
    mult_re = products[0] * factor
    mult_im = products[1] * factor
    data_re = traces[0].astype(jnp.float32)
    data_im = traces[1].astype(jnp.float32)
    sums = lax.psum(
        jnp.stack([
            jnp.sum(mult_re * data_re + mult_im * data_im),
            jnp.sum(mult_re * data_im - mult_im * data_re),
            jnp.sum(mult_re * mult_re + mult_im * mult_im),
        ]),
        ("freq", "shot"),
    )
    return finish(traces, mult_re, mult_im, sums[0], sums[1], sums[2])


def end_schedule(chunks, sizes, ready):
    groups = len(sizes)
    half, most = chunks // 2, 3 * chunks // 4
    done = [0] * chunks
    pieces = []

    def column(c):
        left = sum(sizes[done[c]:])
        if left:
            pieces.append((done[c], groups - done[c], c, 1))
            done[c] = groups
        return left

    window = 2 * sum(sizes)
    room = window - column(0) - column(1)
    following = 2
    while min(done[:most]) < groups:
        while min(done[:most]) < groups:
            group = min(done[:most])
            first = done.index(group)
            bound = half if first < half else most
            last = first
            while last < bound and done[last] == group and (last - first + 1) * sizes[group] <= room:
                last += 1
            if last == first:
                break
            pieces.append((group, 1, first, last - first))
            done[first:last] = [group + 1] * (last - first)
            room -= (last - first) * sizes[group]
        room += window
        if following < chunks:
            room -= column(following)
            following += 1
    step = max(1, (chunks - most) // 2)
    pieces += [(0, groups, c, min(step, chunks - c)) for c in range(most, chunks, step)]
    out = []
    for group, count, first, width in pieces:
        column_need = 2 * (first - 2) + 1
        group_need = min(2 * ready[g] for g in range(group, group + count)) if first < most else chunks - 1
        out.append((group, count, first, width, max(-1, min(column_need, group_need, chunks - 1))))
    return tuple(out)


def line_kernel(
    chunks, kept, sizes, ready, schedule, freqs,
    traces_ref, mult_ref, total_ref,
    grid, stage, acc, packed, partial_in,
    load_sem, piece_send, piece_recv, ici_recv, far_send, end_send, pair_send, pair_recv,
    result_send, result_recv, full_send, full_recv, sum_send, sum_recv,
):
    rows = traces_ref.shape[2]
    order = traces_ref.shape[3]
    groups = len(sizes)
    firsts = [sum(sizes[:g]) for g in range(groups)]
    half, quarter = chunks // 2, chunks // 4
    factor = 1.0 / math.sqrt(order)
    freq = lax.axis_index("freq")
    shot = lax.axis_index("shot")
    z = shot // 2
    core = shot % 2
    low = z < 2
    end = jnp.where(low, 0, 3)
    mid = jnp.where(low, 1, 2)
    far_mid = jnp.where(low, 2, 1)
    far_end = jnp.where(low, 3, 0)
    is_end = z == end
    beside = freq + 1 - 2 * (freq % 2)
    across = (freq + 2) % freqs

    def first_last(i):
        return (i + quarter) % chunks

    def first_third(i):
        return jnp.where(i < half, i + quarter, jnp.where(i < 3 * quarter, i - half, i))

    def sent(i):
        return jnp.where(low, first_last(i), first_third(i))

    def taken(i):
        return jnp.where(low, first_third(i), first_last(i))

    def row(chip, plane):
        return pl.multiple_of((chip * 2 + plane) * rows, rows)

    def lane(j):
        return pl.multiple_of(j * LANES, LANES)

    def block(chip, plane, j):
        return grid.at[:, pl.ds(row(chip, plane), rows), pl.ds(lane(j), LANES)]

    def remote(src, dst, send, recv, chip, plane):
        return pltpu.make_async_remote_copy(
            src_ref=src, dst_ref=dst, send_sem=send, recv_sem=recv,
            device_id=(freq, chip * 2 + plane), device_id_type=MESH,
        )

    def ici(chip, j, send, slot, target):
        ref = block(chip, core, j)
        return remote(ref, ref, send, ici_recv.at[slot, j], target, core)

    def pair(chip, j, slot):
        ref = block(chip, core, j)
        return remote(ref, ref, pair_send.at[slot, j], pair_recv.at[slot, j], z, 1 - core)

    def arrived(chip, j, slot):
        ref = block(chip, core, j)
        remote(ref, ref, far_send.at[0, j], ici_recv.at[slot, j], z, 1 - core).wait_recv()

    def paired(chip, j, slot):
        ref = block(chip, 1 - core, j)
        remote(ref, ref, pair_send.at[slot, j], pair_recv.at[slot, j], z, 1 - core).wait_recv()

    def to_end(chip, j, slot):
        return ici(chip, j, end_send.at[slot, j], slot, end)

    def to_far(chip, j, slot):
        return ici(chip, j, far_send.at[slot, j], slot + 1, far_mid)

    def piece(d):
        group, count, first, width, _ = schedule[d]
        ref = grid.at[
            :,
            pl.ds(pl.multiple_of(row(end, core) + firsts[group], 16), sum(sizes[group:group + count])),
            pl.ds(lane(sent(first)), width * LANES),
        ]
        return remote(ref, ref, piece_send.at[d], piece_recv.at[d], mid, core)

    def result(g, i):
        here = pl.ds(firsts[g], sizes[g])
        return remote(
            stage.at[:, here, pl.ds(lane(i - kept), LANES)],
            mult_ref.at[:, here, pl.ds(lane(taken(i)), LANES)],
            result_send.at[g, i], result_recv.at[g, i], end, core,
        )

    def full(i):
        return remote(
            stage.at[:, :, pl.ds(lane(i - kept), LANES)],
            mult_ref.at[:, :, pl.ds(lane(taken(i)), LANES)],
            full_send.at[i - half], full_recv.at[i - half], end, core,
        )

    def multiply(first, count, j, inner, depth, out, out_row, out_lane, onto, fit):
        here = pl.ds(first, count)
        column = pl.ds(lane(j), LANES)
        span = pl.ds(inner, depth)
        right = jnp.concatenate([grid[0, span, column], grid[1, span, column]], axis=1)
        by_re = jnp.dot(grid[0, here, span], right, preferred_element_type=jnp.float32)
        by_im = jnp.dot(grid[1, here, span], right, preferred_element_type=jnp.float32)
        mult_re = (by_re[:, :LANES] - by_im[:, LANES:]) * factor
        mult_im = (by_re[:, LANES:] + by_im[:, :LANES]) * factor
        to = pl.ds(out_row, count), pl.ds(out_lane, LANES)
        if onto:
            mult_re = mult_re + out[0, to[0], to[1]]
            mult_im = mult_im + out[1, to[0], to[1]]
        out[0, to[0], to[1]] = mult_re
        out[1, to[0], to[1]] = mult_im
        if not fit:
            return
        data_re = grid[0, here, column].astype(jnp.float32)
        data_im = grid[1, here, column].astype(jnp.float32)
        for i, term in enumerate((
            mult_re * data_re + mult_im * data_im,
            mult_re * data_im - mult_im * data_re,
            mult_re * mult_re + mult_im * mult_im,
        )):
            acc[pl.ds(i * 8, 8), :] += jnp.sum(term.reshape(count // 8, 8, LANES), axis=0)

    def own(j):
        multiply(row(z, core), rows, j, 0, order, mult_ref, 0, lane(j), False, True)

    def loop(lower, upper, body):
        def run(j, carry):
            body(j)
            return carry
        lax.fori_loop(lower, upper, run, 0)

    def pack():
        sums = [jnp.sum(acc[pl.ds(8 * i, 8), :], axis=0, keepdims=True) for i in range(3)]
        return jnp.concatenate(sums + [jnp.zeros((5, LANES), jnp.float32)], axis=0)

    def give(slot, device):
        return pltpu.make_async_remote_copy(
            src_ref=packed.at[slot], dst_ref=partial_in.at[slot],
            send_sem=sum_send.at[slot], recv_sem=sum_recv.at[slot],
            device_id=device, device_id_type=MESH,
        )

    def give_total():
        return remote(total_ref, total_ref, sum_send.at[5], sum_recv.at[5], end, core)

    mine = grid.at[:, pl.ds(row(z, core), rows), :]
    load = pltpu.make_async_copy(traces_ref.at[:, 0], mine, load_sem)
    load.start()
    acc[...] = jnp.zeros_like(acc)

    barrier = pltpu.get_barrier_semaphore()

    def greet(f, s):
        pl.semaphore_signal(barrier, inc=1, device_id=(f, s), device_id_type=MESH)

    greet(freq, z * 2 + 1 - core)

    @pl.when(is_end)
    def _():
        greet(freq, mid * 2 + core)
        pl.semaphore_wait(barrier, 2)

    @pl.when(jnp.logical_not(is_end))
    def _():
        greet(freq, end * 2 + core)
        greet(freq, far_mid * 2 + core)
        greet(beside, shot)
        greet(across, shot)
        pl.semaphore_wait(barrier, 5)

    load.wait()

    @pl.when(is_end)
    def _():
        for d in range(len(schedule)):
            piece(d).start()
        loop(0, half, lambda i: pair(z, taken(i), 3).start())

        def work(i):
            j = taken(i)
            for slot, chip in enumerate((mid, far_mid, far_end)):
                arrived(chip, j, slot)
                pair(chip, j, slot).start()
            for slot, chip in enumerate((mid, far_mid, far_end, end)):
                paired(chip, j, slot)
            own(j)

        loop(0, kept, work)

        def complete(i):
            j = taken(i)
            paired(end, j, 3)
            for g in range(groups):
                result(g, i).wait_recv()
            inner = pl.multiple_of(end * 2 * rows, 2 * rows)
            multiply(row(z, core), rows, j, inner, 2 * rows, mult_ref, 0, lane(j), True, True)

        loop(kept, half, complete)
        packed[0] = pack()
        give(0, (freq, mid * 2 + core)).start()

        def settle(i):
            pair(z, taken(i), 3).wait_send()

            @pl.when(i < kept)
            def _():
                for slot, chip in enumerate((mid, far_mid, far_end)):
                    pair(chip, taken(i), slot).wait_send()

        loop(0, half, settle)
        for d in range(len(schedule)):
            piece(d).wait_send()
        give(0, (freq, mid * 2 + core)).wait_send()
        loop(half, chunks, lambda i: full(i).wait_recv())
        give_total().wait_recv()

    @pl.when(jnp.logical_not(is_end))
    def _():
        def own_sends(i):
            to_far(z, sent(i), 0).start()
            pair(z, taken(i), 3).start()

        def near(i):
            to_far(end, sent(i), 1).start()

            @pl.when(i < half)
            def _():
                pair(end, sent(i), 0).start()

        def take_pieces(stop):
            for d in range(len(schedule)):
                @pl.when(stop == schedule[d][4])
                def _(d=d):
                    piece(d).wait_recv()

        lead = min(3, kept)
        own_sends(0)
        own_sends(1)
        loop(0, lead, lambda i: to_end(z, taken(i), 0).start())
        for d in range(len(schedule)):
            if schedule[d][4] < 0:
                piece(d).wait_recv()
        near(0)
        near(1)

        inner = pl.multiple_of((1 - end // 3) * 2 * rows, 2 * rows)

        def part(g, i):
            multiply(
                pl.multiple_of(row(end, core) + firsts[g], 16), sizes[g], taken(i),
                inner, order - 2 * rows, stage, firsts[g], lane(i - kept), False, False,
            )
            result(g, i).start()

        def parts(lowers, uppers):
            for g in range(groups):
                loop(lowers[g], uppers[g], functools.partial(part, g))

        def work(i):
            take_pieces(2 * i)
            parts([kept] * groups, [jnp.where(i == at, i, kept) for at in ready])

            j = taken(i)
            for slot, chip in ((1, far_mid), (2, far_end)):
                arrived(chip, j, slot)

                @pl.when(i < kept)
                def _(slot=slot, chip=chip):
                    to_end(chip, j, slot).start()
                pair(chip, j, slot).start()

            @pl.when(i + lead < kept)
            def _():
                to_end(z, taken(i + lead), 0).start()

            @pl.when(i + 2 < chunks)
            def _():
                own_sends(i + 2)
            for slot, chip in ((0, end), (1, far_mid), (2, far_end), (3, z)):
                paired(chip, j, slot)
            parts([i] * groups, [jnp.where(jnp.logical_and(i >= at, i < half), i + 1, i) for at in ready])

            @pl.when(i >= half)
            def _():
                multiply(row(end, core), rows, j, 0, order, stage, 0, lane(i - kept), False, True)
                full(i).start()
            take_pieces(2 * i + 1)

            @pl.when(i + 2 < chunks)
            def _():
                near(i + 2)

            @pl.when(i == half - 1)
            def _():
                loop(half, chunks, lambda ii: pair(end, sent(ii), 0).start())
            own(j)

        loop(0, chunks, work)

        give(0, (freq, end * 2 + core)).wait_recv()
        total = pack() + partial_in[0]
        for slot, device in enumerate((
            (freq, z * 2 + 1 - core), (freq, far_mid * 2 + core), (beside, shot), (across, shot),
        )):
            packed[slot + 1] = total
            give(slot + 1, device).start()
            give(slot + 1, device).wait_recv()
            total = total + partial_in[slot + 1]
        total_ref[...] = total
        give_total().start()

        def drain(i):
            to_far(z, sent(i), 0).wait_send()
            to_far(end, sent(i), 1).wait_send()
            for slot, chip in enumerate((end, far_mid, far_end, z)):
                pair(chip, taken(i), slot).wait_send()

            @pl.when(i < kept)
            def _():
                for slot, chip in enumerate((z, far_mid, far_end)):
                    to_end(chip, taken(i), slot).wait_send()

            @pl.when(jnp.logical_and(i >= kept, i < half))
            def _():
                for g in range(groups):
                    result(g, i).wait_send()

            @pl.when(i >= half)
            def _():
                full(i).wait_send()

        loop(0, chunks, drain)
        for slot, device in enumerate((
            (freq, z * 2 + 1 - core), (freq, far_mid * 2 + core), (beside, shot), (across, shot),
        )):
            give(slot + 1, device).wait_send()
        give_total().wait_send()


def epilogue_kernel(
    total_count, strip, width, total_ref, traces_ref, mult_ref, multiples_ref, primaries_ref,
    multiples, primaries, fit, sems,
):
    rows, order = mult_ref.shape[1], mult_ref.shape[2]
    num_re, num_im, denom = (jnp.sum(total_ref[pl.ds(i, 1), :]) for i in range(3))
    scaled_den = denom / total_count + epsilon
    fit_re = num_re / total_count / scaled_den
    fit_im = num_im / total_count / scaled_den

    def copies(s):
        here = pl.ds(pl.multiple_of(s * strip, strip), strip)
        return (
            pltpu.make_async_copy(multiples.at[:, here, :], multiples_ref.at[:, 0, here, :], sems.at[0, s]),
            pltpu.make_async_copy(primaries.at[:, here, :], primaries_ref.at[:, 0, here, :], sems.at[1, s]),
        )

    def part(s, carry):
        here = pl.ds(pl.multiple_of(s * strip, strip), strip)
        for q in range(order // width):
            columns = pl.ds(q * width, width)
            mult_re = mult_ref[0, here, columns]
            mult_im = mult_ref[1, here, columns]
            data_re = traces_ref[0, 0, here, columns].astype(jnp.float32)
            data_im = traces_ref[1, 0, here, columns].astype(jnp.float32)
            prim_re = data_re - (fit_re * mult_re - fit_im * mult_im)
            prim_im = data_im - (fit_re * mult_im + fit_im * mult_re)
            multiples[0, here, columns] = mult_re.astype(jnp.bfloat16)
            multiples[1, here, columns] = mult_im.astype(jnp.bfloat16)
            primaries[0, here, columns] = prim_re.astype(jnp.bfloat16)
            primaries[1, here, columns] = prim_im.astype(jnp.bfloat16)
        for copy in copies(s):
            copy.start()
        return carry

    lax.fori_loop(0, rows // strip, part, 0)

    def wait(s, carry):
        for copy in copies(s):
            copy.wait()
        return carry

    lax.fori_loop(0, rows // strip, wait, 0)


def on_a_line(traces):
    rows, order = traces.shape[2], traces.shape[3]
    freqs = lax.axis_size("freq")
    chunks = order // LANES
    half = chunks // 2
    kept = max(1, round(5 * chunks / 24))
    sizes = tuple(part * (rows // 24) for part in (8, 8, 8))
    groups = len(sizes)
    ready = tuple(min(half - 1, max(kept, round(f * chunks / 24))) for f in (5, 6, 8))
    schedule = end_schedule(chunks, sizes, ready)
    pieces = len(schedule)
    dma = pltpu.SemaphoreType.DMA
    mult, totals = pl.pallas_call(
        functools.partial(line_kernel, chunks, kept, sizes, ready, schedule, freqs),
        out_shape=(
            pltpu.VMEM((2, rows, order), jnp.float32),
            pltpu.VMEM((8, LANES), jnp.float32),
        ),
        in_specs=[pl.BlockSpec(memory_space=pltpu.HBM)],
        out_specs=(
            pl.BlockSpec(memory_space=pltpu.VMEM),
            pl.BlockSpec(memory_space=pltpu.VMEM),
        ),
        scratch_shapes=[
            pltpu.VMEM((2, order, order), jnp.bfloat16),
            pltpu.VMEM((2, rows, (chunks - kept) * LANES), jnp.float32),
            pltpu.VMEM((24, LANES), jnp.float32),
            pltpu.VMEM((5, 8, LANES), jnp.float32),
            pltpu.VMEM((5, 8, LANES), jnp.float32),
            dma, dma((pieces,)), dma((pieces,)), dma((3, chunks)), dma((2, chunks)),
            dma((3, chunks)), dma((4, chunks)), dma((4, chunks)),
            dma((groups, half)), dma((groups, half)), dma((half,)), dma((half,)), dma((6,)), dma((6,)),
        ],
        compiler_params=pltpu.CompilerParams(
            collective_id=0, has_side_effects=True, vmem_limit_bytes=48 * 1024 * 1024
        ),
    )(traces)
    strip = 32
    out = jax.ShapeDtypeStruct(traces.shape, traces.dtype)
    whole = pl.BlockSpec(memory_space=pltpu.VMEM)
    away = pl.BlockSpec(memory_space=pltpu.HBM)
    return pl.pallas_call(
        functools.partial(epilogue_kernel, float(freqs * order * order), strip, 4 * LANES),
        out_shape=(out, out),
        in_specs=[whole, whole, whole],
        out_specs=(away, away),
        scratch_shapes=[
            pltpu.VMEM((2, rows, order), jnp.bfloat16),
            pltpu.VMEM((2, rows, order), jnp.bfloat16),
            pltpu.SMEM((2,), jnp.float32),
            dma((2, rows // strip)),
        ],
        compiler_params=pltpu.CompilerParams(vmem_limit_bytes=24 * 1024 * 1024),
    )(totals, traces, mult)


def solution(mesh):
    placed = P(None, "freq", "shot", None)

    def per_device(traces):
        four_chips = mesh.shape["shot"] == 2 * 4 and mesh.shape["freq"] == 4
        rows, order = traces.shape[2], traces.shape[3]
        fits = rows % 384 == 0 and order % (4 * LANES) == 0
        if four_chips and traces.shape[1] == 1 and fits:
            return on_a_line(traces)
        return gathered(traces)

    return jax.shard_map(
        per_device, mesh=mesh, in_specs=(placed,), out_specs=(placed, placed), check_vma=False
    )
```

```python
import functools
import math

import jax
import jax.numpy as jnp
from jax import lax
from jax.experimental import pallas as pl
from jax.experimental.pallas import tpu as pltpu
from jax.sharding import PartitionSpec as P

epsilon = 1e-06
MESH = pl.DeviceIdType.MESH
LANES = 128


def complex_product(left_re, left_im, right):
    left_block = jnp.stack(
        [jnp.concatenate([left_re, -left_im], axis=2), jnp.concatenate([left_im, left_re], axis=2)]
    )
    right_block = jnp.concatenate([right[0], right[1]], axis=1)
    return jnp.einsum("cfik,fkn->cfin", left_block, right_block, preferred_element_type=jnp.float32)


def finish(traces, mult_re, mult_im, num_re, num_im, denom):
    matrix_order = traces.shape[3]
    data_re = traces[0].astype(jnp.float32)
    data_im = traces[1].astype(jnp.float32)
    total_count = float(traces.shape[1] * lax.axis_size("freq") * matrix_order * matrix_order)
    scaled_den = denom / total_count + epsilon
    fit_re = num_re / total_count / scaled_den
    fit_im = num_im / total_count / scaled_den
    prim_re = data_re - (fit_re * mult_re - fit_im * mult_im)
    prim_im = data_im - (fit_re * mult_im + fit_im * mult_re)
    multiples = jnp.stack([mult_re, mult_im]).astype(jnp.bfloat16)
    primaries = jnp.stack([prim_re, prim_im]).astype(jnp.bfloat16)
    return (multiples, primaries)


def gathered(traces):
    factor = 1.0 / math.sqrt(traces.shape[3])
    products = complex_product(
        traces[0], traces[1], lax.all_gather(traces, "shot", axis=2, tiled=True)
    )
    mult_re = products[0] * factor
    mult_im = products[1] * factor
    data_re = traces[0].astype(jnp.float32)
    data_im = traces[1].astype(jnp.float32)
    sums = lax.psum(
        jnp.stack([
            jnp.sum(mult_re * data_re + mult_im * data_im),
            jnp.sum(mult_re * data_im - mult_im * data_re),
            jnp.sum(mult_re * mult_re + mult_im * mult_im),
        ]),
        ("freq", "shot"),
    )
    return finish(traces, mult_re, mult_im, sums[0], sums[1], sums[2])


def end_schedule(chunks, sizes, ready):
    groups = len(sizes)
    half, most = chunks // 2, 3 * chunks // 4
    done = [0] * chunks
    pieces = []

    def column(c):
        left = sum(sizes[done[c]:])
        if left:
            pieces.append((done[c], groups - done[c], c, 1))
            done[c] = groups
        return left

    window = 2 * sum(sizes)
    room = window - column(0) - column(1)
    following = 2
    while min(done[:most]) < groups:
        while min(done[:most]) < groups:
            group = min(done[:most])
            first = done.index(group)
            bound = half if first < half else most
            last = first
            while last < bound and done[last] == group and (last - first + 1) * sizes[group] <= room:
                last += 1
            if last == first:
                break
            pieces.append((group, 1, first, last - first))
            done[first:last] = [group + 1] * (last - first)
            room -= (last - first) * sizes[group]
        room += window
        if following < chunks:
            room -= column(following)
            following += 1
    step = max(1, (chunks - most) // 2)
    pieces += [(0, groups, c, min(step, chunks - c)) for c in range(most, chunks, step)]
    out = []
    for group, count, first, width in pieces:
        column_need = 2 * (first - 2) + 1
        group_need = min(2 * ready[g] for g in range(group, group + count)) if first < most else chunks - 1
        out.append((group, count, first, width, max(-1, min(column_need, group_need, chunks - 1))))
    return tuple(out)


def line_kernel(
    chunks, kept, sizes, ready, schedule, freqs,
    traces_ref, mult_ref, fit_ref,
    grid, stage, acc, packed, partial_in,
    load_sem, piece_send, piece_recv, ici_recv, far_send, end_send, pair_send, pair_recv,
    result_send, result_recv, full_send, full_recv, sum_send, sum_recv,
):
    rows = traces_ref.shape[2]
    order = traces_ref.shape[3]
    groups = len(sizes)
    firsts = [sum(sizes[:g]) for g in range(groups)]
    half, quarter = chunks // 2, chunks // 4
    factor = 1.0 / math.sqrt(order)
    freq = lax.axis_index("freq")
    shot = lax.axis_index("shot")
    z = shot // 2
    core = shot % 2
    low = z < 2
    end = jnp.where(low, 0, 3)
    mid = jnp.where(low, 1, 2)
    far_mid = jnp.where(low, 2, 1)
    far_end = jnp.where(low, 3, 0)
    is_end = z == end
    beside = freq + 1 - 2 * (freq % 2)
    across = (freq + 2) % freqs

    def first_last(i):
        return (i + quarter) % chunks

    def first_third(i):
        return jnp.where(i < half, i + quarter, jnp.where(i < 3 * quarter, i - half, i))

    def sent(i):
        return jnp.where(low, first_last(i), first_third(i))

    def taken(i):
        return jnp.where(low, first_third(i), first_last(i))

    def row(chip, plane):
        return pl.multiple_of((chip * 2 + plane) * rows, rows)

    def lane(j):
        return pl.multiple_of(j * LANES, LANES)

    def block(chip, plane, j):
        return grid.at[:, pl.ds(row(chip, plane), rows), pl.ds(lane(j), LANES)]

    def remote(src, dst, send, recv, chip, plane):
        return pltpu.make_async_remote_copy(
            src_ref=src, dst_ref=dst, send_sem=send, recv_sem=recv,
            device_id=(freq, chip * 2 + plane), device_id_type=MESH,
        )

    def ici(chip, j, send, slot, target):
        ref = block(chip, core, j)
        return remote(ref, ref, send, ici_recv.at[slot, j], target, core)

    def pair(chip, j, slot):
        ref = block(chip, core, j)
        return remote(ref, ref, pair_send.at[slot, j], pair_recv.at[slot, j], z, 1 - core)

    def arrived(chip, j, slot):
        ref = block(chip, core, j)
        remote(ref, ref, far_send.at[0, j], ici_recv.at[slot, j], z, 1 - core).wait_recv()

    def paired(chip, j, slot):
        ref = block(chip, 1 - core, j)
        remote(ref, ref, pair_send.at[slot, j], pair_recv.at[slot, j], z, 1 - core).wait_recv()

    def to_end(chip, j, slot):
        return ici(chip, j, end_send.at[slot, j], slot, end)

    def to_far(chip, j, slot):
        return ici(chip, j, far_send.at[slot, j], slot + 1, far_mid)

    def piece(d):
        group, count, first, width, _ = schedule[d]
        ref = grid.at[
            :,
            pl.ds(pl.multiple_of(row(end, core) + firsts[group], 16), sum(sizes[group:group + count])),
            pl.ds(lane(sent(first)), width * LANES),
        ]
        return remote(ref, ref, piece_send.at[d], piece_recv.at[d], mid, core)

    def result(g, i):
        here = pl.ds(firsts[g], sizes[g])
        return remote(
            stage.at[:, here, pl.ds(lane(i - kept), LANES)],
            mult_ref.at[:, here, pl.ds(lane(taken(i)), LANES)],
            result_send.at[g, i], result_recv.at[g, i], end, core,
        )

    def full(i):
        return remote(
            stage.at[:, :, pl.ds(lane(i - kept), LANES)],
            mult_ref.at[:, :, pl.ds(lane(taken(i)), LANES)],
            full_send.at[i - half], full_recv.at[i - half], end, core,
        )

    def multiply(first, count, j, inner, depth, out, out_row, out_lane, onto, fit):
        here = pl.ds(first, count)
        column = pl.ds(lane(j), LANES)
        span = pl.ds(inner, depth)
        right = jnp.concatenate([grid[0, span, column], grid[1, span, column]], axis=1)
        by_re = jnp.dot(grid[0, here, span], right, preferred_element_type=jnp.float32)
        by_im = jnp.dot(grid[1, here, span], right, preferred_element_type=jnp.float32)
        mult_re = (by_re[:, :LANES] - by_im[:, LANES:]) * factor
        mult_im = (by_re[:, LANES:] + by_im[:, :LANES]) * factor
        to = pl.ds(out_row, count), pl.ds(out_lane, LANES)
        if onto:
            mult_re = mult_re + out[0, to[0], to[1]]
            mult_im = mult_im + out[1, to[0], to[1]]
        out[0, to[0], to[1]] = mult_re
        out[1, to[0], to[1]] = mult_im
        if not fit:
            return
        data_re = grid[0, here, column].astype(jnp.float32)
        data_im = grid[1, here, column].astype(jnp.float32)
        for i, term in enumerate((
            mult_re * data_re + mult_im * data_im,
            mult_re * data_im - mult_im * data_re,
            mult_re * mult_re + mult_im * mult_im,
        )):
            acc[pl.ds(i * 8, 8), :] += jnp.sum(term.reshape(count // 8, 8, LANES), axis=0)

    def own(j):
        multiply(row(z, core), rows, j, 0, order, mult_ref, 0, lane(j), False, True)

    def loop(lower, upper, body):
        def run(j, carry):
            body(j)
            return carry
        lax.fori_loop(lower, upper, run, 0)

    def pack():
        sums = [jnp.sum(acc[pl.ds(8 * i, 8), :], axis=0, keepdims=True) for i in range(3)]
        return jnp.concatenate(sums + [jnp.zeros((5, LANES), jnp.float32)], axis=0)

    def give(slot, device):
        return pltpu.make_async_remote_copy(
            src_ref=packed.at[slot], dst_ref=partial_in.at[slot],
            send_sem=sum_send.at[slot], recv_sem=sum_recv.at[slot],
            device_id=device, device_id_type=MESH,
        )

    def give_fit():
        return remote(fit_ref, fit_ref, sum_send.at[5], sum_recv.at[5], end, core)

    early = min(3, half)

    def load(part):
        first, last = ((quarter, quarter + early), (quarter + early, chunks), (0, quarter))[part]
        columns = pl.ds(first * LANES, (last - first) * LANES)
        return pltpu.make_async_copy(
            traces_ref.at[:, 0, :, columns],
            grid.at[:, pl.ds(row(z, core), rows), columns],
            load_sem.at[part],
        )

    for part in range(3):
        load(part).start()
    acc[...] = jnp.zeros_like(acc)

    barrier = pltpu.get_barrier_semaphore()

    def greet(f, s):
        pl.semaphore_signal(barrier, inc=1, device_id=(f, s), device_id_type=MESH)

    greet(freq, z * 2 + 1 - core)

    @pl.when(is_end)
    def _():
        greet(freq, mid * 2 + core)
        pl.semaphore_wait(barrier, 2)

    @pl.when(jnp.logical_not(is_end))
    def _():
        greet(freq, end * 2 + core)
        greet(freq, far_mid * 2 + core)
        greet(beside, shot)
        greet(across, shot)
        pl.semaphore_wait(barrier, 5)

    load(0).wait()
    at_once = [d for d in range(len(schedule)) if sum(schedule[d][2:4]) <= early]

    @pl.when(is_end)
    def _():
        for d in at_once:
            piece(d).start()
        load(1).wait()
        load(2).wait()
        for d in range(len(schedule)):
            if d not in at_once:
                piece(d).start()
        loop(0, half, lambda i: pair(z, taken(i), 3).start())

        def work(i):
            j = taken(i)
            for slot, chip in enumerate((mid, far_mid, far_end)):
                arrived(chip, j, slot)
                pair(chip, j, slot).start()
            for slot, chip in enumerate((mid, far_mid, far_end, end)):
                paired(chip, j, slot)
            own(j)

        loop(0, kept, work)

        def complete(i):
            j = taken(i)
            paired(end, j, 3)
            for g in range(groups):
                result(g, i).wait_recv()
            inner = pl.multiple_of(end * 2 * rows, 2 * rows)
            multiply(row(z, core), rows, j, inner, 2 * rows, mult_ref, 0, lane(j), True, True)

        loop(kept, half, complete)
        packed[0] = pack()
        give(0, (freq, mid * 2 + core)).start()

        def settle(i):
            pair(z, taken(i), 3).wait_send()

            @pl.when(i < kept)
            def _():
                for slot, chip in enumerate((mid, far_mid, far_end)):
                    pair(chip, taken(i), slot).wait_send()

        loop(0, half, settle)
        for d in range(len(schedule)):
            piece(d).wait_send()
        give(0, (freq, mid * 2 + core)).wait_send()
        loop(half, chunks, lambda i: full(i).wait_recv())
        give_fit().wait_recv()

    @pl.when(jnp.logical_not(is_end))
    def _():
        def own_sends(i):
            to_far(z, sent(i), 0).start()
            pair(z, taken(i), 3).start()

        def near(i):
            to_far(end, sent(i), 1).start()

            @pl.when(i < half)
            def _():
                pair(end, sent(i), 0).start()

        def take_pieces(stop):
            for d in range(len(schedule)):
                @pl.when(stop == schedule[d][4])
                def _(d=d):
                    piece(d).wait_recv()

        lead = min(early, kept)
        own_sends(0)
        own_sends(1)
        loop(0, lead, lambda i: to_end(z, taken(i), 0).start())
        load(1).wait()
        load(2).wait()
        for d in range(len(schedule)):
            if schedule[d][4] < 0:
                piece(d).wait_recv()
        near(0)
        near(1)

        inner = pl.multiple_of((1 - end // 3) * 2 * rows, 2 * rows)

        def part(g, i):
            multiply(
                pl.multiple_of(row(end, core) + firsts[g], 16), sizes[g], taken(i),
                inner, order - 2 * rows, stage, firsts[g], lane(i - kept), False, False,
            )
            result(g, i).start()

        def parts(lowers, uppers):
            for g in range(groups):
                loop(lowers[g], uppers[g], functools.partial(part, g))

        def work(i):
            take_pieces(2 * i)
            parts([kept] * groups, [jnp.where(i == at, i, kept) for at in ready])

            j = taken(i)
            for slot, chip in ((1, far_mid), (2, far_end)):
                arrived(chip, j, slot)

                @pl.when(i < kept)
                def _(slot=slot, chip=chip):
                    to_end(chip, j, slot).start()
                pair(chip, j, slot).start()

            @pl.when(i + lead < kept)
            def _():
                to_end(z, taken(i + lead), 0).start()

            @pl.when(i + 2 < chunks)
            def _():
                own_sends(i + 2)
            for slot, chip in ((0, end), (1, far_mid), (2, far_end), (3, z)):
                paired(chip, j, slot)
            parts([i] * groups, [jnp.where(jnp.logical_and(i >= at, i < half), i + 1, i) for at in ready])

            @pl.when(i >= half)
            def _():
                multiply(row(end, core), rows, j, 0, order, stage, 0, lane(i - kept), False, True)
                full(i).start()
            take_pieces(2 * i + 1)

            @pl.when(i + 2 < chunks)
            def _():
                near(i + 2)

            @pl.when(i == half - 1)
            def _():
                loop(half, chunks, lambda ii: pair(end, sent(ii), 0).start())
            own(j)

        loop(0, chunks, work)

        give(0, (freq, end * 2 + core)).wait_recv()
        total = pack() + partial_in[0]
        for slot, device in enumerate((
            (freq, z * 2 + 1 - core), (freq, far_mid * 2 + core), (beside, shot), (across, shot),
        )):
            packed[slot + 1] = total
            give(slot + 1, device).start()
            give(slot + 1, device).wait_recv()
            total = total + partial_in[slot + 1]
        num_re, num_im, denom = (jnp.sum(total[i:i + 1], axis=1, keepdims=True) for i in range(3))
        total_count = float(freqs * order * order)
        scaled_den = denom / total_count + epsilon
        fit_re = jnp.broadcast_to(num_re / total_count / scaled_den, (1, LANES))
        fit_im = jnp.broadcast_to(num_im / total_count / scaled_den, (1, LANES))
        fit_ref[...] = jnp.concatenate([fit_re, fit_im, jnp.zeros((6, LANES), jnp.float32)], axis=0)
        give_fit().start()

        def drain(i):
            to_far(z, sent(i), 0).wait_send()
            to_far(end, sent(i), 1).wait_send()
            for slot, chip in enumerate((end, far_mid, far_end, z)):
                pair(chip, taken(i), slot).wait_send()

            @pl.when(i < kept)
            def _():
                for slot, chip in enumerate((z, far_mid, far_end)):
                    to_end(chip, taken(i), slot).wait_send()

            @pl.when(jnp.logical_and(i >= kept, i < half))
            def _():
                for g in range(groups):
                    result(g, i).wait_send()

            @pl.when(i >= half)
            def _():
                full(i).wait_send()

        loop(0, chunks, drain)
        for slot, device in enumerate((
            (freq, z * 2 + 1 - core), (freq, far_mid * 2 + core), (beside, shot), (across, shot),
        )):
            give(slot + 1, device).wait_send()
        give_fit().wait_send()


def epilogue_kernel(
    strip, width, fit_ref, traces_ref, mult_ref, multiples_ref, primaries_ref,
    multiples, primaries, sems,
):
    rows, order = mult_ref.shape[1], mult_ref.shape[2]
    spread = width // LANES

    def here(s):
        return pl.ds(pl.multiple_of(s * strip, strip), strip)

    def copy(s, which):
        src, dst = ((multiples, multiples_ref), (primaries, primaries_ref))[which]
        return pltpu.make_async_copy(src.at[:, here(s), :], dst.at[:, 0, here(s), :], sems.at[which, s])

    def round_off(s, carry):
        for q in range(order // width):
            columns = pl.ds(q * width, width)
            for part in range(2):
                multiples[part, here(s), columns] = mult_ref[part, here(s), columns].astype(jnp.bfloat16)
        copy(s, 0).start()
        return carry

    def subtract(s, carry):
        fit_re = jnp.concatenate([fit_ref[0:1, :]] * spread, axis=1)
        fit_im = jnp.concatenate([fit_ref[1:2, :]] * spread, axis=1)
        for q in range(order // width):
            columns = pl.ds(q * width, width)
            mult_re = mult_ref[0, here(s), columns]
            mult_im = mult_ref[1, here(s), columns]
            data_re = traces_ref[0, 0, here(s), columns].astype(jnp.float32)
            data_im = traces_ref[1, 0, here(s), columns].astype(jnp.float32)
            prim_re = data_re - (fit_re * mult_re - fit_im * mult_im)
            prim_im = data_im - (fit_re * mult_im + fit_im * mult_re)
            primaries[0, here(s), columns] = prim_re.astype(jnp.bfloat16)
            primaries[1, here(s), columns] = prim_im.astype(jnp.bfloat16)
        copy(s, 1).start()
        return carry

    def wait(s, carry):
        copy(s, 0).wait()
        copy(s, 1).wait()
        return carry

    for step in (round_off, subtract, wait):
        lax.fori_loop(0, rows // strip, step, 0)


def on_a_line(traces):
    rows, order = traces.shape[2], traces.shape[3]
    freqs = lax.axis_size("freq")
    chunks = order // LANES
    half = chunks // 2
    kept = max(1, round(5 * chunks / 24))
    sizes = tuple(part * (rows // 24) for part in (8, 8, 8))
    groups = len(sizes)
    ready = tuple(min(half - 1, max(kept, round(f * chunks / 24))) for f in (5, 6, 8))
    schedule = end_schedule(chunks, sizes, ready)
    pieces = len(schedule)
    dma = pltpu.SemaphoreType.DMA
    mult, fit = pl.pallas_call(
        functools.partial(line_kernel, chunks, kept, sizes, ready, schedule, freqs),
        out_shape=(
            pltpu.VMEM((2, rows, order), jnp.float32),
            pltpu.VMEM((8, LANES), jnp.float32),
        ),
        in_specs=[pl.BlockSpec(memory_space=pltpu.HBM)],
        out_specs=(
            pl.BlockSpec(memory_space=pltpu.VMEM),
            pl.BlockSpec(memory_space=pltpu.VMEM),
        ),
        scratch_shapes=[
            pltpu.VMEM((2, order, order), jnp.bfloat16),
            pltpu.VMEM((2, rows, (chunks - kept) * LANES), jnp.float32),
            pltpu.VMEM((24, LANES), jnp.float32),
            pltpu.VMEM((5, 8, LANES), jnp.float32),
            pltpu.VMEM((5, 8, LANES), jnp.float32),
            dma((3,)), dma((pieces,)), dma((pieces,)), dma((3, chunks)), dma((2, chunks)),
            dma((3, chunks)), dma((4, chunks)), dma((4, chunks)),
            dma((groups, half)), dma((groups, half)), dma((half,)), dma((half,)), dma((6,)), dma((6,)),
        ],
        compiler_params=pltpu.CompilerParams(
            collective_id=0, has_side_effects=True, vmem_limit_bytes=48 * 1024 * 1024
        ),
    )(traces)
    strip = 32
    out = jax.ShapeDtypeStruct(traces.shape, traces.dtype)
    whole = pl.BlockSpec(memory_space=pltpu.VMEM)
    away = pl.BlockSpec(memory_space=pltpu.HBM)
    return pl.pallas_call(
        functools.partial(epilogue_kernel, strip, 4 * LANES),
        out_shape=(out, out),
        in_specs=[whole, whole, whole],
        out_specs=(away, away),
        scratch_shapes=[
            pltpu.VMEM((2, rows, order), jnp.bfloat16),
            pltpu.VMEM((2, rows, order), jnp.bfloat16),
            dma((2, rows // strip)),
        ],
        compiler_params=pltpu.CompilerParams(vmem_limit_bytes=24 * 1024 * 1024),
    )(fit, traces, mult)


def solution(mesh):
    placed = P(None, "freq", "shot", None)

    def per_device(traces):
        four_chips = mesh.shape["shot"] == 2 * 4 and mesh.shape["freq"] == 4
        rows, order = traces.shape[2], traces.shape[3]
        fits = rows % 384 == 0 and order % (4 * LANES) == 0
        if four_chips and traces.shape[1] == 1 and fits:
            return on_a_line(traces)
        return gathered(traces)

    return jax.shard_map(
        per_device, mesh=mesh, in_specs=(placed,), out_specs=(placed, placed), check_vma=False
    )
```

```python
import functools
import math

import jax
import jax.numpy as jnp
from jax import lax
from jax.experimental import pallas as pl
from jax.experimental.pallas import tpu as pltpu
from jax.sharding import PartitionSpec as P

epsilon = 1e-06
MESH = pl.DeviceIdType.MESH
LANES = 128


def complex_product(left_re, left_im, right):
    left_block = jnp.stack(
        [jnp.concatenate([left_re, -left_im], axis=2), jnp.concatenate([left_im, left_re], axis=2)]
    )
    right_block = jnp.concatenate([right[0], right[1]], axis=1)
    return jnp.einsum("cfik,fkn->cfin", left_block, right_block, preferred_element_type=jnp.float32)


def finish(traces, mult_re, mult_im, num_re, num_im, denom):
    matrix_order = traces.shape[3]
    data_re = traces[0].astype(jnp.float32)
    data_im = traces[1].astype(jnp.float32)
    total_count = float(traces.shape[1] * lax.axis_size("freq") * matrix_order * matrix_order)
    scaled_den = denom / total_count + epsilon
    fit_re = num_re / total_count / scaled_den
    fit_im = num_im / total_count / scaled_den
    prim_re = data_re - (fit_re * mult_re - fit_im * mult_im)
    prim_im = data_im - (fit_re * mult_im + fit_im * mult_re)
    multiples = jnp.stack([mult_re, mult_im]).astype(jnp.bfloat16)
    primaries = jnp.stack([prim_re, prim_im]).astype(jnp.bfloat16)
    return (multiples, primaries)


def gathered(traces):
    factor = 1.0 / math.sqrt(traces.shape[3])
    products = complex_product(
        traces[0], traces[1], lax.all_gather(traces, "shot", axis=2, tiled=True)
    )
    mult_re = products[0] * factor
    mult_im = products[1] * factor
    data_re = traces[0].astype(jnp.float32)
    data_im = traces[1].astype(jnp.float32)
    sums = lax.psum(
        jnp.stack([
            jnp.sum(mult_re * data_re + mult_im * data_im),
            jnp.sum(mult_re * data_im - mult_im * data_re),
            jnp.sum(mult_re * mult_re + mult_im * mult_im),
        ]),
        ("freq", "shot"),
    )
    return finish(traces, mult_re, mult_im, sums[0], sums[1], sums[2])


def end_schedule(chunks, sizes, ready):
    groups = len(sizes)
    half, most = chunks // 2, 3 * chunks // 4
    done = [0] * chunks
    pieces = []

    def column(c):
        left = sum(sizes[done[c]:])
        if left:
            pieces.append((done[c], groups - done[c], c, 1))
            done[c] = groups
        return left

    window = 2 * sum(sizes)
    room = window - column(0) - column(1)
    following = 2
    while min(done[:most]) < groups:
        while min(done[:most]) < groups:
            group = min(done[:most])
            first = done.index(group)
            bound = half if first < half else most
            last = first
            while last < bound and done[last] == group and (last - first + 1) * sizes[group] <= room:
                last += 1
            if last == first:
                break
            pieces.append((group, 1, first, last - first))
            done[first:last] = [group + 1] * (last - first)
            room -= (last - first) * sizes[group]
        room += window
        if following < chunks:
            room -= column(following)
            following += 1
    step = max(1, (chunks - most) // 2)
    pieces += [(0, groups, c, min(step, chunks - c)) for c in range(most, chunks, step)]
    out = []
    for group, count, first, width in pieces:
        column_need = 2 * (first - 2) + 1
        group_need = min(2 * ready[g] for g in range(group, group + count)) if first < most else chunks - 1
        out.append((group, count, first, width, max(-1, min(column_need, group_need, chunks - 1))))
    return tuple(out)


def line_kernel(
    chunks, kept, sizes, ready, schedule, freqs,
    traces_ref, mult_ref, fit_ref, mine_ref,
    grid, stage, acc, packed, partial_in,
    load_sem, piece_send, piece_recv, ici_recv, far_send, end_send, pair_send, pair_recv,
    result_send, result_recv, full_send, full_recv, sum_send, sum_recv,
):
    rows = traces_ref.shape[2]
    order = traces_ref.shape[3]
    groups = len(sizes)
    firsts = [sum(sizes[:g]) for g in range(groups)]
    half, quarter = chunks // 2, chunks // 4
    factor = 1.0 / math.sqrt(order)
    freq = lax.axis_index("freq")
    shot = lax.axis_index("shot")
    z = shot // 2
    core = shot % 2
    low = z < 2
    end = jnp.where(low, 0, 3)
    mid = jnp.where(low, 1, 2)
    far_mid = jnp.where(low, 2, 1)
    far_end = jnp.where(low, 3, 0)
    is_end = z == end
    beside = freq + 1 - 2 * (freq % 2)
    across = (freq + 2) % freqs

    def first_last(i):
        return (i + quarter) % chunks

    def first_third(i):
        return jnp.where(i < half, i + quarter, jnp.where(i < 3 * quarter, i - half, i))

    def sent(i):
        return jnp.where(low, first_last(i), first_third(i))

    def taken(i):
        return jnp.where(low, first_third(i), first_last(i))

    def row(chip, plane):
        return pl.multiple_of((chip * 2 + plane) * rows, rows)

    def lane(j):
        return pl.multiple_of(j * LANES, LANES)

    def block(chip, plane, j):
        return grid.at[:, pl.ds(row(chip, plane), rows), pl.ds(lane(j), LANES)]

    def remote(src, dst, send, recv, chip, plane):
        return pltpu.make_async_remote_copy(
            src_ref=src, dst_ref=dst, send_sem=send, recv_sem=recv,
            device_id=(freq, chip * 2 + plane), device_id_type=MESH,
        )

    def ici(chip, j, send, slot, target):
        ref = block(chip, core, j)
        return remote(ref, ref, send, ici_recv.at[slot, j], target, core)

    def pair(chip, j, slot):
        ref = block(chip, core, j)
        return remote(ref, ref, pair_send.at[slot, j], pair_recv.at[slot, j], z, 1 - core)

    def arrived(chip, j, slot):
        ref = block(chip, core, j)
        remote(ref, ref, far_send.at[0, j], ici_recv.at[slot, j], z, 1 - core).wait_recv()

    def paired(chip, j, slot):
        ref = block(chip, 1 - core, j)
        remote(ref, ref, pair_send.at[slot, j], pair_recv.at[slot, j], z, 1 - core).wait_recv()

    def to_end(chip, j, slot):
        return ici(chip, j, end_send.at[slot, j], slot, end)

    def to_far(chip, j, slot):
        return ici(chip, j, far_send.at[slot, j], slot + 1, far_mid)

    def piece(d):
        group, count, first, width, _ = schedule[d]
        ref = grid.at[
            :,
            pl.ds(pl.multiple_of(row(end, core) + firsts[group], 16), sum(sizes[group:group + count])),
            pl.ds(lane(sent(first)), width * LANES),
        ]
        return remote(ref, ref, piece_send.at[d], piece_recv.at[d], mid, core)

    def result(g, i):
        here = pl.ds(firsts[g], sizes[g])
        return remote(
            stage.at[:, here, pl.ds(lane(i - kept), LANES)],
            mult_ref.at[:, here, pl.ds(lane(taken(i)), LANES)],
            result_send.at[g, i], result_recv.at[g, i], end, core,
        )

    def full(i):
        return remote(
            stage.at[:, :, pl.ds(lane(i - kept), LANES)],
            mult_ref.at[:, :, pl.ds(lane(taken(i)), LANES)],
            full_send.at[i - half], full_recv.at[i - half], end, core,
        )

    def multiply(first, count, j, inner, depth, out, out_row, out_lane, onto, fit):
        here = pl.ds(first, count)
        column = pl.ds(lane(j), LANES)
        span = pl.ds(inner, depth)
        right = jnp.concatenate([grid[0, span, column], grid[1, span, column]], axis=1)
        by_re = jnp.dot(grid[0, here, span], right, preferred_element_type=jnp.float32)
        by_im = jnp.dot(grid[1, here, span], right, preferred_element_type=jnp.float32)
        mult_re = (by_re[:, :LANES] - by_im[:, LANES:]) * factor
        mult_im = (by_re[:, LANES:] + by_im[:, :LANES]) * factor
        to = pl.ds(out_row, count), pl.ds(out_lane, LANES)
        if onto:
            mult_re = mult_re + out[0, to[0], to[1]]
            mult_im = mult_im + out[1, to[0], to[1]]
        out[0, to[0], to[1]] = mult_re
        out[1, to[0], to[1]] = mult_im
        if not fit:
            return
        data_re = grid[0, here, column].astype(jnp.float32)
        data_im = grid[1, here, column].astype(jnp.float32)
        for i, term in enumerate((
            mult_re * data_re + mult_im * data_im,
            mult_re * data_im - mult_im * data_re,
            mult_re * mult_re + mult_im * mult_im,
        )):
            acc[pl.ds(i * 8, 8), :] += jnp.sum(term.reshape(count // 8, 8, LANES), axis=0)

    def own(j):
        multiply(row(z, core), rows, j, 0, order, mult_ref, 0, lane(j), False, True)

    def loop(lower, upper, body):
        def run(j, carry):
            body(j)
            return carry
        lax.fori_loop(lower, upper, run, 0)

    def pack():
        sums = [jnp.sum(acc[pl.ds(8 * i, 8), :], axis=0, keepdims=True) for i in range(3)]
        return jnp.concatenate(sums + [jnp.zeros((5, LANES), jnp.float32)], axis=0)

    def give(slot, device):
        return pltpu.make_async_remote_copy(
            src_ref=packed.at[slot], dst_ref=partial_in.at[slot],
            send_sem=sum_send.at[slot], recv_sem=sum_recv.at[slot],
            device_id=device, device_id_type=MESH,
        )

    def give_fit():
        return remote(fit_ref, fit_ref, sum_send.at[5], sum_recv.at[5], end, core)

    early = min(3, half)

    def load(part):
        first, last = ((quarter, quarter + early), (quarter + early, chunks), (0, quarter))[part]
        columns = pl.ds(first * LANES, (last - first) * LANES)
        return pltpu.make_async_copy(
            traces_ref.at[:, 0, :, columns],
            grid.at[:, pl.ds(row(z, core), rows), columns],
            load_sem.at[part],
        )

    for part in range(3):
        load(part).start()
    acc[...] = jnp.zeros_like(acc)

    barrier = pltpu.get_barrier_semaphore()

    def greet(f, s):
        pl.semaphore_signal(barrier, inc=1, device_id=(f, s), device_id_type=MESH)

    greet(freq, z * 2 + 1 - core)

    @pl.when(is_end)
    def _():
        greet(freq, mid * 2 + core)
        pl.semaphore_wait(barrier, 2)

    @pl.when(jnp.logical_not(is_end))
    def _():
        greet(freq, end * 2 + core)
        greet(freq, far_mid * 2 + core)
        greet(beside, shot)
        greet(across, shot)
        pl.semaphore_wait(barrier, 5)

    again = pltpu.make_async_copy(traces_ref.at[:, 0], mine_ref, load_sem.at[3])
    load(0).wait()
    at_once = [d for d in range(len(schedule)) if sum(schedule[d][2:4]) <= early]

    @pl.when(is_end)
    def _():
        for d in at_once:
            piece(d).start()
        load(1).wait()
        load(2).wait()
        again.start()
        for d in range(len(schedule)):
            if d not in at_once:
                piece(d).start()
        loop(0, half, lambda i: pair(z, taken(i), 3).start())

        def work(i):
            j = taken(i)
            for slot, chip in enumerate((mid, far_mid, far_end)):
                arrived(chip, j, slot)
                pair(chip, j, slot).start()
            for slot, chip in enumerate((mid, far_mid, far_end, end)):
                paired(chip, j, slot)
            own(j)

        loop(0, kept, work)

        def complete(i):
            j = taken(i)
            paired(end, j, 3)
            for g in range(groups):
                result(g, i).wait_recv()
            inner = pl.multiple_of(end * 2 * rows, 2 * rows)
            multiply(row(z, core), rows, j, inner, 2 * rows, mult_ref, 0, lane(j), True, True)

        loop(kept, half, complete)
        packed[0] = pack()
        give(0, (freq, mid * 2 + core)).start()

        def settle(i):
            pair(z, taken(i), 3).wait_send()

            @pl.when(i < kept)
            def _():
                for slot, chip in enumerate((mid, far_mid, far_end)):
                    pair(chip, taken(i), slot).wait_send()

        loop(0, half, settle)
        for d in range(len(schedule)):
            piece(d).wait_send()
        give(0, (freq, mid * 2 + core)).wait_send()
        loop(half, chunks, lambda i: full(i).wait_recv())
        give_fit().wait_recv()
        again.wait()

    @pl.when(jnp.logical_not(is_end))
    def _():
        def own_sends(i):
            to_far(z, sent(i), 0).start()
            pair(z, taken(i), 3).start()

        def near(i):
            to_far(end, sent(i), 1).start()

            @pl.when(i < half)
            def _():
                pair(end, sent(i), 0).start()

        def take_pieces(stop):
            for d in range(len(schedule)):
                @pl.when(stop == schedule[d][4])
                def _(d=d):
                    piece(d).wait_recv()

        lead = min(early, kept)
        own_sends(0)
        own_sends(1)
        loop(0, lead, lambda i: to_end(z, taken(i), 0).start())
        load(1).wait()
        load(2).wait()
        again.start()
        for d in range(len(schedule)):
            if schedule[d][4] < 0:
                piece(d).wait_recv()
        near(0)
        near(1)

        inner = pl.multiple_of((1 - end // 3) * 2 * rows, 2 * rows)

        def part(g, i):
            multiply(
                pl.multiple_of(row(end, core) + firsts[g], 16), sizes[g], taken(i),
                inner, order - 2 * rows, stage, firsts[g], lane(i - kept), False, False,
            )
            result(g, i).start()

        def parts(lowers, uppers):
            for g in range(groups):
                loop(lowers[g], uppers[g], functools.partial(part, g))

        def work(i):
            take_pieces(2 * i)
            parts([kept] * groups, [jnp.where(i == at, i, kept) for at in ready])

            j = taken(i)
            for slot, chip in ((1, far_mid), (2, far_end)):
                arrived(chip, j, slot)

                @pl.when(i < kept)
                def _(slot=slot, chip=chip):
                    to_end(chip, j, slot).start()
                pair(chip, j, slot).start()

            @pl.when(i + lead < kept)
            def _():
                to_end(z, taken(i + lead), 0).start()

            @pl.when(i + 2 < chunks)
            def _():
                own_sends(i + 2)
            for slot, chip in ((0, end), (1, far_mid), (2, far_end), (3, z)):
                paired(chip, j, slot)
            parts([i] * groups, [jnp.where(jnp.logical_and(i >= at, i < half), i + 1, i) for at in ready])

            @pl.when(i >= half)
            def _():
                multiply(row(end, core), rows, j, 0, order, stage, 0, lane(i - kept), False, True)
                full(i).start()
            take_pieces(2 * i + 1)

            @pl.when(i + 2 < chunks)
            def _():
                near(i + 2)

            @pl.when(i == half - 1)
            def _():
                loop(half, chunks, lambda ii: pair(end, sent(ii), 0).start())
            own(j)

        loop(0, chunks, work)

        give(0, (freq, end * 2 + core)).wait_recv()
        total = pack() + partial_in[0]
        for slot, device in enumerate((
            (freq, z * 2 + 1 - core), (freq, far_mid * 2 + core), (beside, shot), (across, shot),
        )):
            packed[slot + 1] = total
            give(slot + 1, device).start()
            give(slot + 1, device).wait_recv()
            total = total + partial_in[slot + 1]
        num_re, num_im, denom = (jnp.sum(total[i:i + 1], axis=1, keepdims=True) for i in range(3))
        total_count = float(freqs * order * order)
        scaled_den = denom / total_count + epsilon
        fit_re = jnp.broadcast_to(num_re / total_count / scaled_den, (1, LANES))
        fit_im = jnp.broadcast_to(num_im / total_count / scaled_den, (1, LANES))
        fit_ref[...] = jnp.concatenate([fit_re, fit_im, jnp.zeros((6, LANES), jnp.float32)], axis=0)
        give_fit().start()
        again.wait()

        def drain(i):
            to_far(z, sent(i), 0).wait_send()
            to_far(end, sent(i), 1).wait_send()
            for slot, chip in enumerate((end, far_mid, far_end, z)):
                pair(chip, taken(i), slot).wait_send()

            @pl.when(i < kept)
            def _():
                for slot, chip in enumerate((z, far_mid, far_end)):
                    to_end(chip, taken(i), slot).wait_send()

            @pl.when(jnp.logical_and(i >= kept, i < half))
            def _():
                for g in range(groups):
                    result(g, i).wait_send()

            @pl.when(i >= half)
            def _():
                full(i).wait_send()

        loop(0, chunks, drain)
        for slot, device in enumerate((
            (freq, z * 2 + 1 - core), (freq, far_mid * 2 + core), (beside, shot), (across, shot),
        )):
            give(slot + 1, device).wait_send()
        give_fit().wait_send()


def epilogue_kernel(
    strip, width, fit_ref, mine_ref, mult_ref, multiples_ref, primaries_ref,
    multiples, primaries, sems,
):
    rows, order = mult_ref.shape[1], mult_ref.shape[2]
    spread = width // LANES

    def here(s):
        return pl.ds(pl.multiple_of(s * strip, strip), strip)

    def copy(s, which):
        src, dst = ((multiples, multiples_ref), (primaries, primaries_ref))[which]
        return pltpu.make_async_copy(src.at[:, here(s), :], dst.at[:, 0, here(s), :], sems.at[which, s])

    def round_off(s, carry):
        for q in range(order // width):
            columns = pl.ds(q * width, width)
            for part in range(2):
                multiples[part, here(s), columns] = mult_ref[part, here(s), columns].astype(jnp.bfloat16)
        copy(s, 0).start()
        return carry

    def subtract(s, carry):
        fit_re = jnp.concatenate([fit_ref[0:1, :]] * spread, axis=1)
        fit_im = jnp.concatenate([fit_ref[1:2, :]] * spread, axis=1)
        for q in range(order // width):
            columns = pl.ds(q * width, width)
            mult_re = mult_ref[0, here(s), columns]
            mult_im = mult_ref[1, here(s), columns]
            data_re = mine_ref[0, here(s), columns].astype(jnp.float32)
            data_im = mine_ref[1, here(s), columns].astype(jnp.float32)
            prim_re = data_re - (fit_re * mult_re - fit_im * mult_im)
            prim_im = data_im - (fit_re * mult_im + fit_im * mult_re)
            primaries[0, here(s), columns] = prim_re.astype(jnp.bfloat16)
            primaries[1, here(s), columns] = prim_im.astype(jnp.bfloat16)
        copy(s, 1).start()
        return carry

    def wait(s, carry):
        copy(s, 0).wait()
        copy(s, 1).wait()
        return carry

    for step in (round_off, subtract, wait):
        lax.fori_loop(0, rows // strip, step, 0)


def on_a_line(traces):
    rows, order = traces.shape[2], traces.shape[3]
    freqs = lax.axis_size("freq")
    chunks = order // LANES
    half = chunks // 2
    kept = max(1, round(5 * chunks / 24))
    sizes = tuple(part * (rows // 24) for part in (8, 8, 8))
    groups = len(sizes)
    ready = tuple(min(half - 1, max(kept, round(f * chunks / 24))) for f in (5, 6, 8))
    schedule = end_schedule(chunks, sizes, ready)
    pieces = len(schedule)
    dma = pltpu.SemaphoreType.DMA
    mult, fit, mine = pl.pallas_call(
        functools.partial(line_kernel, chunks, kept, sizes, ready, schedule, freqs),
        out_shape=(
            pltpu.VMEM((2, rows, order), jnp.float32),
            pltpu.VMEM((8, LANES), jnp.float32),
            pltpu.VMEM((2, rows, order), jnp.bfloat16),
        ),
        in_specs=[pl.BlockSpec(memory_space=pltpu.HBM)],
        out_specs=(pl.BlockSpec(memory_space=pltpu.VMEM),) * 3,
        scratch_shapes=[
            pltpu.VMEM((2, order, order), jnp.bfloat16),
            pltpu.VMEM((2, rows, (chunks - kept) * LANES), jnp.float32),
            pltpu.VMEM((24, LANES), jnp.float32),
            pltpu.VMEM((5, 8, LANES), jnp.float32),
            pltpu.VMEM((5, 8, LANES), jnp.float32),
            dma((4,)), dma((pieces,)), dma((pieces,)), dma((3, chunks)), dma((2, chunks)),
            dma((3, chunks)), dma((4, chunks)), dma((4, chunks)),
            dma((groups, half)), dma((groups, half)), dma((half,)), dma((half,)), dma((6,)), dma((6,)),
        ],
        compiler_params=pltpu.CompilerParams(
            collective_id=0, has_side_effects=True, vmem_limit_bytes=48 * 1024 * 1024
        ),
    )(traces)
    strip = 32
    out = jax.ShapeDtypeStruct(traces.shape, traces.dtype)
    whole = pl.BlockSpec(memory_space=pltpu.VMEM)
    away = pl.BlockSpec(memory_space=pltpu.HBM)
    return pl.pallas_call(
        functools.partial(epilogue_kernel, strip, 4 * LANES),
        out_shape=(out, out),
        in_specs=[whole, whole, whole],
        out_specs=(away, away),
        scratch_shapes=[
            pltpu.VMEM((2, rows, order), jnp.bfloat16),
            pltpu.VMEM((2, rows, order), jnp.bfloat16),
            dma((2, rows // strip)),
        ],
        compiler_params=pltpu.CompilerParams(vmem_limit_bytes=24 * 1024 * 1024),
    )(fit, mine, mult)


def solution(mesh):
    placed = P(None, "freq", "shot", None)

    def per_device(traces):
        four_chips = mesh.shape["shot"] == 2 * 4 and mesh.shape["freq"] == 4
        rows, order = traces.shape[2], traces.shape[3]
        fits = rows % 384 == 0 and order % (4 * LANES) == 0
        if four_chips and traces.shape[1] == 1 and fits:
            return on_a_line(traces)
        return gathered(traces)

    return jax.shard_map(
        per_device, mesh=mesh, in_specs=(placed,), out_specs=(placed, placed), check_vma=False
    )
```
